256 devices in a mesh: outer: 16 (over z_hi, x, core), chip: 16 (over y, z_lo).
Axes of the slice: x: 4, y: 4, z: 8 (z_hi: 2, z_lo: 4; z = z_hi * 4 + z_lo), core: 2. Of those that a mesh axis runs over, the one named last changes fastest.
Arguments:
- inputs: bfloat16 [32768, 2048], P(('outer', 'chip')), may hold values from -6 to 6
- out_grads: bfloat16 [32768, 2048], P(('outer', 'chip')), may hold values from -6 to 6
- weight: bfloat16 [2048, 2048], P('chip'), may hold values from -0.125 to 0.125
- start_basis: float32 [128, 2048], P('chip'), may hold values from -6 to 6
- error_buffer: float32 [16, 2048, 2048], P('outer', 'chip'), may hold values from -2 to 2
Outputs:
- outputs: bfloat16 [32768, 2048], P(('outer', 'chip'))
- new_error: float32 [16, 2048, 2048], P('outer', 'chip')
The draws below stay inside these ranges and needn't reach their ends.
All inputs are finite; a program needn't handle non-finite values.
Results may differ from the reference program's by a relative error of at most 0.0085.
Values may be sent and summed in bfloat16 or wider, within the bound.
A program may use at most 128 MiB of HBM per device.

```python
import jax
import jax.numpy as jnp
from jax import lax

D = 2048
INNER = 2048
RANK = 8
TOK_DEV = 128
PODS = 16
QROWS = 128
TOKENS = 32768
N_CHIP = 16


def block_levels(own_key, extent, shards, least, high):
    def one(position, parts):
        draws = jax.random.uniform(jax.random.fold_in(jax.random.fold_in(own_key, 6), position), (parts,), jnp.float32, least / len(shards), high / len(shards))
        return jnp.repeat(jnp.exp(draws), extent[position] // parts).reshape((-1,) + (1,) * (len(extent) - position - 1))

    factor_of = one(*shards[0])
    for cut in shards[1:]:
        factor_of = factor_of * one(*cut)
    return factor_of


def centred(key, extent, scale, reach, shards=(), kind=jnp.bfloat16):
    level = block_levels(key, extent, shards, -0.22, 0.18) if shards else 1.0
    array = jax.random.normal(key, extent, jnp.float32) * scale * level
    return jnp.minimum(jnp.maximum(array, -reach), reach).astype(kind)


def setup_inputs(seed: int = 0) -> dict:
    keys = jax.random.split(jax.random.key(seed), 6)
    return {
        "inputs": centred(keys[0], (TOKENS, D), 1.0, 6.0, ((0, 256),)),
        "out_grads": centred(keys[1], (TOKENS, INNER), 1.0, 6.0, ((0, 256),)),
        "weight": centred(keys[2], (D, INNER), D ** -0.5, 0.125, ((0, 16),)),
        "start_basis": centred(keys[3], (QROWS, INNER), 1.0, 6.0, ((0, 16),), jnp.float32),
        "error_buffer": centred(keys[4], (PODS, D, INNER), 0.25, 2.0, ((0, 16), (1, 16)), jnp.float32),
    }


LEARNING_RATE = 0.2

def orthonormal(projected):
    finished = []
    for index in range(projected.shape[-2]):
        vector = projected[..., index, :]
        for unit in finished:
            vector = vector - lax.optimization_barrier(jnp.sum(vector * unit, axis=-1, keepdims=True)) * unit
        finished.append(vector / jnp.sqrt(lax.optimization_barrier(jnp.sum(vector * vector, axis=-1, keepdims=True)) + 1.0))
    return jnp.stack(finished, axis=-2)

def reference(inputs, out_grads, weight, start_basis, error_buffer):
    highest = lax.Precision.HIGHEST
    shard_rows = D // N_CHIP
    pod_tokens = TOK_DEV * N_CHIP
    basis_in = start_basis.reshape(N_CHIP, RANK, INNER)
    merged_all = []
    left_sum = jnp.zeros((N_CHIP, RANK, shard_rows), jnp.float32)
    for pod in range(PODS):
        pod_inputs = inputs[pod * pod_tokens:(pod + 1) * pod_tokens]
        pod_grads = out_grads[pod * pod_tokens:(pod + 1) * pod_tokens]
        gradient = lax.dot_general(pod_inputs, pod_grads, (((0,), (0,)), ((), ())), preferred_element_type=jnp.float32) / TOK_DEV
        merged = (gradient + error_buffer[pod]).reshape(N_CHIP, shard_rows, INNER)
        merged_all.append(merged)
        left_sum = left_sum + jnp.einsum('cki,cri->ckr', basis_in, merged, precision=highest)
    left_basis = orthonormal(left_sum / PODS)
    right_sum = jnp.zeros((N_CHIP, RANK, INNER), jnp.float32)
    for merged in merged_all:
        right_sum = right_sum + jnp.einsum('ckr,cri->cki', left_basis, merged, precision=highest)
    right_factor = right_sum / PODS
    approx = jnp.einsum('ckr,cki->cri', left_basis, right_factor, precision=highest)
    new_error = jnp.stack([merged - approx for merged in merged_all]).reshape(PODS, D, INNER)
    new_weight = (weight.astype(jnp.float32) - LEARNING_RATE * approx.reshape(D, INNER)).astype(jnp.bfloat16)
    outputs = jnp.dot(inputs, new_weight, preferred_element_type=jnp.float32).astype(jnp.bfloat16)
    return (outputs, new_error)
```

```python
import jax
import jax.numpy as jnp
from jax import lax
from jax.experimental import pallas as pl
from jax.experimental.pallas import tpu as pltpu
from jax.sharding import Mesh
from jax.sharding import PartitionSpec as P

MESH_ID = pl.DeviceIdType.MESH
AXES = ("zh", "x", "core", "y", "z")
LEARNING_RATE = 0.2
TOK = 128
D = 2048
NCH = 8
CW = D // NCH
F32 = jnp.float32
BF16 = jnp.bfloat16


def body(
    x_hbm, g_hbm, w_hbm, b_hbm, e_hbm, out_hbm, ne_hbm,
    xx, xp, xgt, dyb, wg, eb, bb, pf, sb, rl, rr, mg, xo, xw, lf, lall, rt, rsb, rall, ob,
    ld_x, ld_g, ld_w, ld_b, ld_e,
    wz_s, wz_r, wy_s, wy_r, wc_s, wc_r, xp_s, xp_r, xx_s, xx_r,
    dy_s, dy_r, re_s, re_r, rs_s, rsl_r, rsr_r,
    lf_s, lf_r, la_s, la_r, rt_s, rt_r, ro_s, ro_r, rc_s, rc_r, xo_s, xo_r,
    ne_s, out_s,
):
    zh, x, core, y, z = (lax.axis_index(a) for a in AXES)
    outer = (zh * 4 + x) * 2 + core
    sl = x * 2 + core
    c = y * 4 + z

    def remote(src, dst, ssem, rsem, dev):
        return pltpu.make_async_remote_copy(
            src_ref=src, dst_ref=dst, send_sem=ssem, recv_sem=rsem,
            device_id=dev, device_id_type=MESH_ID,
        )

    def outer_dev(o):
        return {"zh": o // 8, "x": (o // 2) % 4, "core": o % 2}

    def chip_dev(k):
        return {"y": k // 4, "z": k % 4}

    yp, ym = (y + 1) % 4, (y + 3) % 4
    y2 = (y + 2) % 4

    w_ld = pltpu.make_async_copy(w_hbm.at[:, pl.ds(pl.multiple_of(sl * CW, CW), CW)], wg.at[core, y, z], ld_w.at[0])
    w_ld.start()
    x_ld = [pltpu.make_async_copy(x_hbm.at[:, pl.ds(q * 512, 512)], xx.at[x, q], ld_x.at[q]) for q in range(4)]
    for cp in x_ld:
        cp.start()
    g_ld = [pltpu.make_async_copy(g_hbm.at[:, pl.ds(n * CW, CW)], dyb.at[n, y], ld_g.at[n]) for n in range(NCH)]
    for cp in g_ld:
        cp.start()
    b_ld = [pltpu.make_async_copy(b_hbm.at[:, pl.ds(n * CW, CW)], bb.at[n], ld_b.at[n]) for n in range(NCH)]
    e_ld = [pltpu.make_async_copy(e_hbm.at[0, :, pl.ds(n * CW, CW)], eb.at[n], ld_e.at[n]) for n in range(NCH)]
    for cp in b_ld + e_ld:
        cp.start()

    barrier = pltpu.get_barrier_semaphore()

    @pl.loop(1, 16)
    def _(i):
        pl.semaphore_signal(barrier, inc=1, device_id=outer_dev((outer + i) % 16), device_id_type=MESH_ID)
        pl.semaphore_signal(barrier, inc=1, device_id=chip_dev((c + i) % 16), device_id_type=MESH_ID)

    pl.semaphore_wait(barrier, 30)

    def wz_copy(p):
        return remote(wg.at[core, y, z], wg.at[core, y, z], wz_s.at[p], wz_r.at[z], {"z": p})

    def wz_recv(p):
        return remote(wg.at[core, y, p], wg.at[core, y, p], wz_s.at[p], wz_r.at[p], {"z": p})

    def wy_copy(p):
        return remote(wg.at[core, y], wg.at[core, y], wy_s.at[p], wy_r.at[y], {"y": p})

    def wy_recv(p):
        return remote(wg.at[core, p], wg.at[core, p], wy_s.at[p], wy_r.at[p], {"y": p})

    def wc_copy():
        return remote(wg.at[core], wg.at[core], wc_s.at[0], wc_r.at[0], {"core": 1 - core})

    def wc_recv():
        return remote(wg.at[1 - core], wg.at[1 - core], wc_s.at[0], wc_r.at[0], {"core": 1 - core})

    def xp_copy(p):
        return remote(xx.at[x, p], xp.at[y], xp_s.at[p], xp_r.at[y], {"y": p})

    def xp_recv(p):
        return remote(xx.at[x, p], xp.at[p], xp_s.at[p], xp_r.at[p], {"y": p})

    def xx_copy(p):
        return remote(xx.at[x], xx.at[x], xx_s.at[p], xx_r.at[x], {"x": p})

    def xx_recv(p):
        return remote(xx.at[p], xx.at[p], xx_s.at[p], xx_r.at[p], {"x": p})

    def dy_copy(d, n):
        return remote(dyb.at[n, y], dyb.at[n, y], dy_s.at[d, n], dy_r.at[d, n], {"y": yp if d == 0 else ym})

    def dy_recv(d, n):
        src = ym if d == 0 else yp
        return remote(dyb.at[n, src], dyb.at[n, src], dy_s.at[d, n], dy_r.at[d, n], {"y": yp})

    def relay(n, up):
        blk = ym if up else yp
        return remote(dyb.at[n, blk], dyb.at[n, blk], re_s.at[n], re_r.at[n], {"y": yp if up else ym})

    def relay_recv(n):
        return remote(dyb.at[n, y2], dyb.at[n, y2], re_s.at[n], re_r.at[n], {"y": yp})

    def do_relay(n):
        for d in range(2):
            dy_recv(d, n).wait_recv()

        @pl.when(n % 2 == 0)
        def _():
            relay(n, True).start()

        @pl.when(n % 2 == 1)
        def _():
            relay(n, False).start()

    w_ld.wait()
    for i in range(1, 4):
        wz_copy((z + i) % 4).start()
    for cp in x_ld:
        cp.wait()
    for i in (1, 3, 2):
        xp_copy((y + i) % 4).start()
    for n in range(NCH):
        g_ld[n].wait()
        for d in range(2):
            dy_copy(d, n).start()
    for i in (1, 3, 2):
        xx_copy((x + i) % 4).start()
    for cp in b_ld + e_ld:
        cp.wait()

    for i in range(4):
        @pl.when(y == i)
        def _():
            xgt[:, pl.ds(i * TOK, TOK)] = xx[x, i].T

        @pl.when(y != i)
        def _():
            xp_recv(i).wait_recv()
            xgt[:, pl.ds(i * TOK, TOK)] = xp[i].T

    do_relay(0)
    do_relay(1)

    lf[outer] = jnp.zeros((8, TOK), F32)

    @pl.loop(0, NCH + 3)
    def _(s):
        @pl.when(s + 2 < NCH)
        def _():
            do_relay(s + 2)

        @pl.when(s == 2)
        def _():
            for i in range(1, 4):
                wz_recv((z + i) % 4).wait_recv()
            for i in (1, 3, 2):
                wy_copy((y + i) % 4).start()

        @pl.when(s == 7)
        def _():
            for i in range(1, 4):
                wy_recv((y + i) % 4).wait_recv()
            wc_copy().start()

        @pl.when(s < NCH)
        def _():
            relay_recv(s).wait_recv()
            part = jnp.dot(xgt[...], dyb[s].reshape(512, CW), preferred_element_type=F32)
            pf[s] = part.reshape(4, TOK, CW)

        jr = s - z
        jl = s - (3 - z)
        for d in (3, 2, 1):
            @pl.when((jr >= 0) & (jr < NCH) & (d > z))
            def _():
                cp = remote(sb.at[jr, d], rl.at[jr, d], rs_s.at[jr, d], rsl_r.at[jr, d], {"z": (z + 1) % 4})

                @pl.when(z == 0)
                def _():
                    sb[jr, d] = pf[jr, d].astype(BF16)

                @pl.when(z > 0)
                def _():
                    cp.wait_recv()
                    sb[jr, d] = (pf[jr, d] + rl[jr, d].astype(F32)).astype(BF16)

                cp.start()
        for d in (0, 1, 2):
            @pl.when((jl >= 0) & (jl < NCH) & (d < z))
            def _():
                cp = remote(sb.at[jl, d], rr.at[jl, d], rs_s.at[jl, d], rsr_r.at[jl, d], {"z": (z + 3) % 4})

                @pl.when(z == 3)
                def _():
                    sb[jl, d] = pf[jl, d].astype(BF16)

                @pl.when(z < 3)
                def _():
                    cp.wait_recv()
                    sb[jl, d] = (pf[jl, d] + rr[jl, d].astype(F32)).astype(BF16)

                cp.start()

        @pl.when(s >= 3)
        def _():
            n = s - 3
            mg[n] = pf[n, z]

            @pl.when(z > 0)
            def _():
                remote(sb.at[n, z], rl.at[n, z], rs_s.at[n, z], rsl_r.at[n, z], {"z": (z + 1) % 4}).wait_recv()
                mg[n] = mg[n] + rl[n, z].astype(F32)

            @pl.when(z < 3)
            def _():
                remote(sb.at[n, z], rr.at[n, z], rs_s.at[n, z], rsr_r.at[n, z], {"z": (z + 3) % 4}).wait_recv()
                mg[n] = mg[n] + rr[n, z].astype(F32)

            m = mg[n] * (1.0 / TOK) + eb[n]
            mg[n] = m
            lf[outer] = lf[outer] + lax.dot_general(
                bb[n], m, (((1,), (1,)), ((), ())), precision=lax.Precision.HIGHEST, preferred_element_type=F32
            )

    def lf_copy(o, own):
        return remote(lf.at[own], lf.at[own], lf_s.at[o], lf_r.at[own], outer_dev(o))

    @pl.loop(1, 16)
    def _(i):
        lf_copy((outer + i) % 16, outer).start()

    for i in range(1, 4):
        xx_recv((x + i) % 4).wait_recv()
    wc_recv().wait_recv()
    for h in range(2):
        acc = jnp.zeros((512, CW), F32)
        for q in range(4):
            acc = acc + jnp.dot(
                xx[:, q].reshape(512, 512), wg[h, q].reshape(512, CW), preferred_element_type=F32
            )
        xo[:, h] = acc.reshape(4, TOK, CW).astype(BF16)

    def xo_copy(p):
        return remote(xo.at[p], xw.at[x], xo_s.at[p], xo_r.at[x], {"x": p})

    def xo_recv(p):
        return remote(xo.at[p], xw.at[p], xo_s.at[p], xo_r.at[p], {"x": p})

    for i in (1, 3, 2):
        xo_copy((x + i) % 4).start()
    xw[x] = xo[x]

    @pl.loop(1, 16)
    def _(i):
        p = (outer + i) % 16
        lf_copy(p, p).wait_recv()

    v = jnp.sum(lf[...], axis=0) * (1.0 / 16)
    rows = lax.broadcasted_iota(jnp.int32, (8, TOK), 0)
    for k in range(8):
        row = v[k:k + 1]
        dots = jnp.sum(v * row, axis=-1, keepdims=True)
        norm = jnp.sqrt(dots[k:k + 1] + 1.0)
        unit = row / norm
        v = jnp.where(rows > k, v - (dots / norm) * unit, jnp.where(rows == k, unit, v))
    lall[c] = v

    def la_copy(p, own):
        return remote(lall.at[own], lall.at[own], la_s.at[p], la_r.at[own], chip_dev(p))

    vh = v.astype(BF16)
    for n in range(NCH):
        rt[n] = jnp.dot(vh, mg[n].astype(BF16), preferred_element_type=F32).astype(BF16)

    def rt_copy(o):
        return remote(rt.at[o % 8], rsb.at[outer], rt_s.at[o], rt_r.at[outer], outer_dev(o))

    def rt_recv(o):
        return remote(rt.at[o % 8], rsb.at[o], rt_s.at[o], rt_r.at[o], outer_dev(o))

    @pl.loop(1, 16)
    def _(i):
        rt_copy((outer + i) % 16).start()

    rsb[outer] = rt[sl]

    @pl.loop(1, 16)
    def _(i):
        la_copy((c + i) % 16, c).start()

    @pl.loop(1, 16)
    def _(i):
        rt_recv((outer + i) % 16).wait_recv()

    rall[c, sl] = (jnp.sum(rsb[...].astype(F32), axis=0) * (1.0 / 16)).astype(BF16)

    def ro_copy(t, own):
        return remote(rall.at[c, own], rall.at[c, own], ro_s.at[t], ro_r.at[own], {"x": t // 2, "core": t % 2})

    @pl.loop(1, 8)
    def _(i):
        ro_copy((sl + i) % 8, sl).start()

    @pl.loop(1, 16)
    def _(i):
        p = (c + i) % 16
        la_copy(p, p).wait_recv()

    lmat = lall[...].reshape(TOK, TOK)
    lrow = lax.broadcasted_iota(jnp.int32, (TOK, TOK), 0) // 8
    t = jnp.zeros((TOK, TOK), F32)
    for q in range(4):
        lq = jnp.concatenate(
            [jnp.where(lrow == q * 4 + j, lmat, 0.0).astype(BF16) for j in range(4)], axis=1
        )
        t = t + lax.dot_general(xx[x, q], lq, (((1,), (1,)), ((), ())), preferred_element_type=F32)
    t = (t * (-LEARNING_RATE)).astype(BF16)

    @pl.loop(1, 8)
    def _(i):
        p = (sl + i) % 8
        ro_copy(p, p).wait_recv()

    def rc_copy(p, own):
        return remote(rall.at[own], rall.at[own], rc_s.at[p], rc_r.at[own], chip_dev(p))

    @pl.loop(1, 16)
    def _(i):
        rc_copy((c + i) % 16, c).start()

    vt = v.T
    vt_hi = vt.astype(BF16)
    vt_lo = (vt - vt_hi.astype(F32)).astype(BF16)
    for n in range(NCH):
        rn = rall[c, n]
        approx = jnp.dot(vt_hi, rn, preferred_element_type=F32) + jnp.dot(vt_lo, rn, preferred_element_type=F32)
        mg[n] = mg[n] - approx
        pltpu.make_async_copy(mg.at[n], ne_hbm.at[0, :, pl.ds(n * CW, CW)], ne_s.at[n]).start()

    for i in range(1, 4):
        xo_recv((x + i) % 4).wait_recv()

    @pl.loop(1, 16)
    def _(i):
        p = (c + i) % 16
        rc_copy(p, p).wait_recv()

    for n in range(NCH):
        rn = rall[:, n].astype(F32).reshape(TOK, CW).astype(BF16)
        ob[n] = (xw[n // 2, n % 2].astype(F32) + jnp.dot(t, rn, preferred_element_type=F32)).astype(BF16)
        pltpu.make_async_copy(ob.at[n], out_hbm.at[:, pl.ds(n * CW, CW)], out_s.at[n]).start()

    for i in range(1, 4):
        wz_copy((z + i) % 4).wait_send()
        wy_copy((y + i) % 4).wait_send()
        xp_copy((y + i) % 4).wait_send()
        xx_copy((x + i) % 4).wait_send()
        xo_copy((x + i) % 4).wait_send()
    wc_copy().wait_send()

    @pl.loop(0, NCH)
    def _(n):
        dy_copy(0, n).wait_send()
        dy_copy(1, n).wait_send()
        relay(n, True).wait_send()
        for d in range(4):
            @pl.when(d != z)
            def _():
                remote(sb.at[n, d], rl.at[n, d], rs_s.at[n, d], rsl_r.at[n, d], {"z": (z + 1) % 4}).wait_send()

    @pl.loop(1, 16)
    def _(i):
        lf_copy((outer + i) % 16, outer).wait_send()
        rt_copy((outer + i) % 16).wait_send()
        la_copy((c + i) % 16, c).wait_send()
        rc_copy((c + i) % 16, c).wait_send()

    @pl.loop(1, 8)
    def _(i):
        ro_copy((sl + i) % 8, sl).wait_send()

    for n in range(NCH):
        pltpu.make_async_copy(mg.at[n], ne_hbm.at[0, :, pl.ds(n * CW, CW)], ne_s.at[n]).wait()
        pltpu.make_async_copy(ob.at[n], out_hbm.at[:, pl.ds(n * CW, CW)], out_s.at[n]).wait()


def step(inputs, out_grads, weight, start_basis, error_buffer):
    vm = pltpu.VMEM
    dma = pltpu.SemaphoreType.DMA
    return pl.pallas_call(
        body,
        out_shape=(
            jax.ShapeDtypeStruct((TOK, D), BF16),
            jax.ShapeDtypeStruct((1, TOK, D), F32),
        ),
        in_specs=[pl.BlockSpec(memory_space=pl.ANY)] * 5,
        out_specs=(pl.BlockSpec(memory_space=pl.ANY),) * 2,
        scratch_shapes=[
            vm((4, 4, TOK, 512), BF16),
            vm((4, TOK, 512), BF16),
            vm((512, 512), BF16),
            vm((NCH, 4, TOK, CW), BF16),
            vm((2, 4, 4, TOK, CW), BF16),
            vm((NCH, TOK, CW), F32),
            vm((NCH, 8, CW), F32),
            vm((NCH, 4, TOK, CW), F32),
            vm((NCH, 4, TOK, CW), BF16),
            vm((NCH, 4, TOK, CW), BF16),
            vm((NCH, 4, TOK, CW), BF16),
            vm((NCH, TOK, CW), F32),
            vm((4, 2, TOK, CW), BF16),
            vm((4, 2, TOK, CW), BF16),
            vm((16, 8, TOK), F32),
            vm((16, 8, TOK), F32),
            vm((NCH, 8, CW), BF16),
            vm((16, 8, CW), BF16),
            vm((16, NCH, 8, CW), BF16),
            vm((NCH, TOK, CW), BF16),
            dma((4,)), dma((NCH,)), dma((1,)), dma((NCH,)), dma((NCH,)),
            dma((4,)), dma((4,)), dma((4,)), dma((4,)), dma((1,)), dma((1,)),
            dma((4,)), dma((4,)), dma((4,)), dma((4,)),
            dma((2, NCH)), dma((2, NCH)), dma((NCH,)), dma((NCH,)),
            dma((NCH, 4)), dma((NCH, 4)), dma((NCH, 4)),
            dma((16,)), dma((16,)), dma((16,)), dma((16,)), dma((16,)), dma((16,)),
            dma((8,)), dma((8,)), dma((16,)), dma((16,)), dma((4,)), dma((4,)),
            dma((NCH,)), dma((NCH,)),
        ],
        compiler_params=pltpu.CompilerParams(
            collective_id=0, has_side_effects=True, vmem_limit_bytes=60 * 1024 * 1024
        ),
    )(inputs, out_grads, weight, start_basis, error_buffer)


def solution(mesh):
    finer = Mesh(mesh.devices.reshape(2, 4, 2, 4, 4), AXES)
    outer = ("zh", "x", "core")
    chip = ("y", "z")
    in_specs = (
        P(outer + chip, None),
        P(outer + chip, None),
        P(chip, None),
        P(chip, None),
        P(outer, chip, None),
    )
    out_specs = (P(outer + chip, None), P(outer, chip, None))
    return jax.shard_map(step, mesh=finer, in_specs=in_specs, out_specs=out_specs, check_vma=False)
```

```python
import jax
import jax.numpy as jnp
from jax import lax
from jax.experimental import pallas as pl
from jax.experimental.pallas import tpu as pltpu
from jax.sharding import Mesh
from jax.sharding import PartitionSpec as P

MESH_ID = pl.DeviceIdType.MESH
AXES = ("zh", "x", "core", "y", "z")
LEARNING_RATE = 0.2
TOK = 128
D = 2048
NC = 16
CW = D // NC
NS = 8
SW = D // NS
LAG = 2
WZ, WD, WR, WC, XP, XR, XF, XX, DY, RE, RS, LF, LA, RT, RO, RC, RD, XO, NE, OUT = range(20)
XR2, RO2 = 18, 19
OUTER_PEERS = [(h, i, k) for h in (1, 0) for i in (2, 1, 3, 0) for k in (0, 1) if (h, i, k) != (0, 0, 0)]
CHIP_PEERS = [(j, k) for j in (2, 1, 3, 0) for k in (3, 1, 2, 0) if (j, k) != (0, 0)]
F32 = jnp.float32
BF16 = jnp.bfloat16


def body(
    x_hbm, g_hbm, w_hbm, b_hbm, e_hbm, out_hbm, ne_hbm,
    xx, xp, xr, xgt, dyb, wy, wo, eb, bb, pf, sb, rl, rr, mg, xo, xw, lf, lall, rt, rsb, rall, ob,
    ld, snd, got, xp_r, wd_r, dy_r, re_r, rs_r, rz_r, rc_r,
):
    zh, x, core, y, z = (lax.axis_index(a) for a in AXES)
    outer = (zh * 4 + x) * 2 + core
    sl = x * 2 + core
    c = y * 4 + z

    def remote(src, dst, ssem, rsem, dev):
        return pltpu.make_async_remote_copy(
            src_ref=src, dst_ref=dst, send_sem=ssem, recv_sem=rsem,
            device_id=dev, device_id_type=MESH_ID,
        )

    def outer_dev(o):
        return {"zh": (zh + o[0]) % 2, "x": (x + o[1]) % 4, "core": (core + o[2]) % 2}

    def outer_at(o):
        dev = outer_dev(o)
        return (dev["zh"] * 4 + dev["x"]) * 2 + dev["core"]

    def chip_dev(k):
        return {"y": (y + k[0]) % 4, "z": (z + k[1]) % 4}

    def chip_at(k):
        dev = chip_dev(k)
        return dev["y"] * 4 + dev["z"]

    ring = ((y + 1) % 4, (y + 3) % 4)
    y2 = (y + 2) % 4
    near = (3, 1)
    z_up, z_down = (z + 1) % 4, (z + 3) % 4

    barrier = pltpu.get_barrier_semaphore()
    for dev in OUTER_PEERS:
        pl.semaphore_signal(barrier, inc=1, device_id=outer_dev(dev), device_id_type=MESH_ID)
    for dev in CHIP_PEERS:
        pl.semaphore_signal(barrier, inc=1, device_id=chip_dev(dev), device_id_type=MESH_ID)

    w_ld = pltpu.make_async_copy(w_hbm.at[:, pl.ds(pl.multiple_of(sl * SW, SW), SW)], wy.at[z, 0], ld.at[0])
    w_ld.start()
    x_ld = [pltpu.make_async_copy(x_hbm.at[:, pl.ds(q * TOK, TOK)], xx.at[x, q], ld.at[1]) for q in range(16)]
    for q in (3, 0, 7, 4, 11, 8, 15, 12, 2, 1, 6, 5, 10, 9, 14, 13):
        x_ld[q].start()
    g_ld = [pltpu.make_async_copy(g_hbm.at[:, pl.ds(n * CW, CW)], dyb.at[n, 0], ld.at[2]) for n in range(NC)]
    for cp in g_ld:
        cp.start()
    b_ld = [pltpu.make_async_copy(b_hbm.at[:, pl.ds(n * CW, CW)], bb.at[n], ld.at[3]) for n in range(NC)]
    e_ld = [pltpu.make_async_copy(e_hbm.at[0, :, pl.ds(n * CW, CW)], eb.at[n], ld.at[4]) for n in range(NC)]
    for cp in b_ld + e_ld:
        cp.start()

    def arrived(ref, sem):
        remote(ref, ref, snd.at[0], sem, {"core": 1 - core}).wait_recv()

    def gone(ref, kind):
        remote(ref, ref, snd.at[kind], got.at[0], {"core": 1 - core}).wait_send()

    w_ld.wait()
    for i, ref in enumerate((xx.at[x], dyb.at[:, 0], bb, eb)):
        arrived(ref, ld.at[1 + i])
    with jax.named_scope("entry_barrier"):
        pl.semaphore_wait(barrier, 30)

    def wz_copy(p):
        return remote(wy.at[z, 0], wy.at[z, 0], snd.at[WZ], got.at[WZ], {"z": p})

    def wd_copy(way, j):
        return remote(wy.at[j, 0], wy.at[j, near[way]], snd.at[WD], wd_r.at[j], {"y": ring[way]})

    def wr_copy(j, way):
        return remote(wy.at[j, near[way]], wy.at[j, 2], snd.at[WR], got.at[WR], {"y": ring[way]})

    def wc_copy():
        return remote(wy, wo, snd.at[WC], got.at[WC], {"core": 1 - core})

    def xp_copy(way, d):
        p = ring[way]
        return remote(xx.at[x, p * 4 + d], xp.at[near[way], d], snd.at[XP], xp_r.at[0, int(d % 3 > 0)], {"y": p})

    def xr_copy(d):
        way = 0 if d >= 2 else 1
        return remote(xx.at[x, y2 * 4 + d], xr.at[d], snd.at[XR], got.at[XR2 if d % 3 else XR], {"y": ring[way]})

    def xf_copy(d):
        way = 0 if d >= 2 else 1
        return remote(xr.at[d], xp.at[2, d], snd.at[XF], xp_r.at[1, int(d % 3 > 0)], {"y": ring[way]})

    def xx_copy(p):
        return remote(xx.at[x], xx.at[x], snd.at[XX], got.at[XX], {"x": p})

    def dy_copy(way, n):
        return remote(dyb.at[n, 0], dyb.at[n, near[way]], snd.at[DY], dy_r.at[n], {"y": ring[way]})

    def relay(n, way):
        return remote(dyb.at[n, near[way]], dyb.at[n, 2], snd.at[RE], re_r.at[n], {"y": ring[way]})

    def direct(n):
        for way in range(2):
            dy_copy(way, n).start()

    def pass_on(n):
        with jax.named_scope("direct_wait"):
            arrived(dyb.at[n, pl.ds(0, 2)], dy_r.at[n])
        for way in range(2):
            @pl.when(n % 2 == way)
            def _():
                relay(n, way).start()

    def send_x(ds):
        for d in ds:
            for way in range(2):
                xp_copy(way, d).start()

    def pass_x(ds):
        with jax.named_scope("xr_wait"):
            arrived(xr.at[pl.ds(0, 2)], got.at[XR2 if ds[0] % 3 else XR])
        for d in ds:
            xf_copy(d).start()

    def gather_x(ds, slots):
        far = int(slots == (2,))
        if slots != (0,):
            with jax.named_scope("xp_wait"):
                arrived(xr.at[pl.ds(0, 2 if far else 4)], xp_r.at[far, int(ds[0] % 3 > 0)])
        for k in slots:
            for d in ds:
                piece = xp[k, d] if k else xx[x, y * 4 + d]
                xgt[d, :, pl.ds(k * TOK, TOK)] = piece.T

    def product(n, ds):
        block = dyb[n].reshape(4 * TOK, CW)
        for d in ds:
            pf[n, d] = jnp.dot(xgt[d], block, preferred_element_type=F32)

    def send_right(n, d):
        cp = remote(sb.at[n, d], rl.at[n, d], snd.at[RS], rs_r.at[n, d], {"z": z_up})

        @pl.when(z == 0)
        def _():
            sb[n, d] = pf[n, d].astype(BF16)

        @pl.when(z > 0)
        def _():
            with jax.named_scope("right_wait"):
                cp.wait_recv()
            sb[n, d] = (pf[n, d] + rl[n, d].astype(F32)).astype(BF16)

        cp.start()

    def send_left(n, d, h):
        def copy(sem):
            return remote(sb.at[n, d], rr.at[n, d], snd.at[RS], sem, {"z": z_down})


        @pl.when(z == 3)
        def _():
            sb[n, d] = pf[n, d].astype(BF16)

        @pl.when(z < 3)
        def _():
            with jax.named_scope("left_wait"):
                copy(rs_r.at[n, d]).wait_recv()
            sb[n, d] = (pf[n, d] + rr[n, d].astype(F32)).astype(BF16)

        if h > 1:
            copy(rs_r.at[n, d]).start()
        else:
            copy(rz_r.at[n]).start()

    def xo_copy(p):
        return remote(xo.at[p], xw.at[x], snd.at[XO], got.at[XO], {"x": p})

    for i in range(1, 4):
        wz_copy((z + i) % 4).start()
    for d in (3, 0):
        xr_copy(d).start()
    direct(0)
    send_x((3, 0))
    direct(1)
    for i in (1, 3, 2):
        xx_copy((x + i) % 4).start()
    gather_x((3, 0), (0,))
    pass_x((3, 0))
    pass_on(0)
    direct(2)
    gather_x((3, 0), (1, 3))
    pass_on(1)
    direct(3)
    gather_x((3, 0), (2,))
    with jax.named_scope("relay_wait"):
        relay(0, 0).wait_recv()
    with jax.named_scope("product"):
        product(0, (3, 0))

    @pl.when(z == 0)
    def _():
        send_right(0, 3)

    @pl.when(z == 3)
    def _():
        send_left(0, 0, 3)

    pass_on(2)
    direct(4)
    for d in (2, 1):
        xr_copy(d).start()
    send_x((2, 1))
    direct(5)
    gather_x((2, 1), (0,))

    lf[outer] = jnp.zeros((8, TOK), F32)

    @pl.loop(0, NC + 3 * LAG)
    def _(s):
        @pl.when((s >= 1) & (s + 2 < NC))
        def _():
            pass_on(s + 2)

        @pl.when((s >= 1) & (s + 5 < NC))
        def _():
            direct(s + 5)

        @pl.when(s == LAG)
        def _():
            gather_x((2, 1), (1, 3))
            gather_x((2, 1), (2,))

        @pl.when(s == 1)
        def _():
            with jax.named_scope("wz_wait"):
                arrived(wy.at[pl.ds(0, 3), 0], got.at[WZ])

        @pl.when((s >= 11) & (s < 15))
        def _():
            for way in range(2):
                wd_copy(way, s - 11).start()

        for way in range(2):
            @pl.when((s >= 14) & (s < 18) & (s % 2 == way))
            def _():
                j = s - 14
                with jax.named_scope("wd_wait"):
                    arrived(wy.at[j, pl.ds(0, 2)], wd_r.at[j])
                wr_copy(j, way).start()

        @pl.when(s == NC + 4)
        def _():
            with jax.named_scope("wr_wait"):
                arrived(wy.at[:, 2], got.at[WR])
            wc_copy().start()

        @pl.when((s >= 1) & (s < NC))
        def _():
            with jax.named_scope("relay_wait"):
                relay(s, 0).wait_recv()
            with jax.named_scope("product"):
                product(s, (3, 0))

        @pl.when((s >= LAG) & (s < NC + LAG))
        def _():
            with jax.named_scope("product"):
                product(s - LAG, (2, 1))

        for h in (3, 2, 1):
            n = s - LAG * (3 - h)
            ready = (n >= 0) & (n < NC)
            if h == 3:
                ready = ready & (n > 0)

            @pl.when(ready & (z + h < 4))
            def _():
                send_right(n, z + h)

            @pl.when(ready & (z - h >= 0))
            def _():
                send_left(n, z - h, h)

        @pl.when(s == 1)
        def _():
            pass_x((2, 1))

        @pl.when(s >= 3 * LAG)
        def _():
            n = s - 3 * LAG
            mg[n] = pf[n, z]

            @pl.when(z > 0)
            def _():
                with jax.named_scope("last_wait"):
                    remote(sb.at[n, z], rl.at[n, z], snd.at[RS], rs_r.at[n, z], {"z": z_up}).wait_recv()
                mg[n] = mg[n] + rl[n, z].astype(F32)

            @pl.when(z < 3)
            def _():
                with jax.named_scope("last_wait"):
                    remote(sb.at[n, z], rr.at[n, z], snd.at[RS], rz_r.at[n], {"z": z_down}).wait_recv()
                mg[n] = mg[n] + rr[n, z].astype(F32)

            with jax.named_scope("merge"):
                m = mg[n] * (1.0 / TOK) + eb[n]
                mg[n] = m
                lf[outer] = lf[outer] + lax.dot_general(
                    bb[n], m, (((1,), (1,)), ((), ())), precision=lax.Precision.HIGHEST, preferred_element_type=F32
                )

    def lf_copy(i, own):
        o = OUTER_PEERS[i]
        return remote(lf.at[own], lf.at[own], snd.at[LF], got.at[LF], outer_dev(o))

    for i in range(15):
        lf_copy(i, outer).start()

    with jax.named_scope("xx_wait"):
        arrived(xx.at[pl.ds(0, 3)], got.at[XX])
    with jax.named_scope("wc_wait"):
        wc_copy().wait_recv()
    with jax.named_scope("inputs_weight"):
        for h, half in ((core, wy), (1 - core, wo)):
            acc = jnp.zeros((512, SW), F32)
            for j in range(4):
                left = jnp.concatenate([xx[:, ((y + k) % 4) * 4 + j].reshape(512, TOK) for k in range(4)], axis=1)
                acc = acc + jnp.dot(left, half[j].reshape(512, SW), preferred_element_type=F32)
            xo[:, h] = acc.reshape(4, TOK, SW).astype(BF16)
    xw[x] = xo[x]

    with jax.named_scope("lf_wait"):
        arrived(lf.at[pl.ds(0, 15)], got.at[LF])

    with jax.named_scope("gram_schmidt"):
        v = jnp.sum(lf[...], axis=0) * (1.0 / 16)
        rows = lax.broadcasted_iota(jnp.int32, (8, TOK), 0)
        for k in range(8):
            row = v[k:k + 1]
            dots = jnp.sum(v * row, axis=-1, keepdims=True)
            norm = jnp.sqrt(dots[k:k + 1] + 1.0)
            unit = row / norm
            v = jnp.where(rows > k, v - (dots / norm) * unit, jnp.where(rows == k, unit, v))
        lall[c] = v

    def la_copy(i, own):
        return remote(lall.at[own], lall.at[own], snd.at[LA], got.at[LA], chip_dev(CHIP_PEERS[i]))

    with jax.named_scope("right_product"):
        vh = v.astype(BF16)
        for n in range(NC):
            rt[n // 2, :, pl.ds((n % 2) * CW, CW)] = jnp.dot(
                vh, mg[n].astype(BF16), preferred_element_type=F32
            ).astype(BF16)

    def rt_copy(i, to, own):
        return remote(rt.at[to % 8], rsb.at[own], snd.at[RT], got.at[RT], outer_dev(OUTER_PEERS[i]))

    for i in range(15):
        rt_copy(i, outer_at(OUTER_PEERS[i]), outer).start()

    rsb[outer] = rt[sl]

    with jax.named_scope("rt_wait"):
        arrived(rsb.at[pl.ds(0, 15)], got.at[RT])

    rall[c, sl] = (jnp.sum(rsb[...].astype(F32), axis=0) * (1.0 / 16)).astype(BF16)

    def ro_copy(i, own, sem):
        return remote(rall.at[c, own], rall.at[c, own], snd.at[RO], got.at[sem], outer_dev(OUTER_PEERS[i]))

    for i in range(8, 15):
        hands_on = outer_dev(OUTER_PEERS[i])["core"] == x // 2

        @pl.when(hands_on)
        def _():
            ro_copy(i, sl, RO).start()

        @pl.when(jnp.logical_not(hands_on))
        def _():
            ro_copy(i, sl, RO2).start()
    for i in (1, 3, 2):
        xo_copy((x + i) % 4).start()
    for i in range(15):
        la_copy(i, c).start()

    def half_of(k):
        return pl.ds(k * 4, 4)

    def rc_copy(i, own):
        part = rall.at[own, half_of(core)]
        return remote(part, part, snd.at[RC], rc_r.at[own], chip_dev(CHIP_PEERS[i]))

    def rd_copy(own, k):
        part = rall.at[own, half_of(k)]
        return remote(part, part, snd.at[RD], got.at[RD], {"core": 1 - core})

    def ro_wait(sem, with_own):
        with jax.named_scope("ro_wait"):
            @pl.when(with_own)
            def _():
                arrived(rall.at[c, pl.ds(0, 3)], got.at[sem])

            @pl.when(jnp.logical_not(with_own))
            def _():
                arrived(rall.at[c, pl.ds(0, 4)], got.at[sem])

    ro_wait(RO, x // 2 == core)
    for i in range(15):
        rc_copy(i, c).start()
    ro_wait(RO2, x // 2 != core)

    with jax.named_scope("new_error"):
        vt = v.T
        vt_hi = vt.astype(BF16)
        vt_lo = (vt - vt_hi.astype(F32)).astype(BF16)
        for n in range(NC):
            rn = rall[c, n // 2, :, pl.ds((n % 2) * CW, CW)]
            approx = jnp.dot(vt_hi, rn, preferred_element_type=F32) + jnp.dot(vt_lo, rn, preferred_element_type=F32)
            mg[n] = mg[n] - approx
            pltpu.make_async_copy(mg.at[n], ne_hbm.at[0, :, pl.ds(n * CW, CW)], snd.at[NE]).start()

    with jax.named_scope("la_wait"):
        arrived(lall.at[pl.ds(0, 15)], got.at[LA])

    with jax.named_scope("inputs_left"):
        lmat = lall[...].reshape(TOK, TOK)
        lrow = lax.broadcasted_iota(jnp.int32, (TOK, TOK), 0) // 8
        t = jnp.zeros((TOK, TOK), F32)
        for q in range(4):
            lq = jnp.concatenate(
                [jnp.where(lrow == q * 4 + j, lmat, 0.0).astype(BF16) for j in range(4)], axis=1
            )
            xq = jnp.concatenate([xx[x, q * 4 + j] for j in range(4)], axis=1)
            t = t + lax.dot_general(xq, lq, (((1,), (1,)), ((), ())), preferred_element_type=F32)
        t = (t * (-LEARNING_RATE)).astype(BF16)

    with jax.named_scope("rc_wait"):
        for i in reversed(range(15)):
            p = chip_at(CHIP_PEERS[i])
            rc_copy(i, p).wait_recv()
            rd_copy(p, core).start()
    with jax.named_scope("rd_wait"):
        arrived(rall.at[pl.ds(0, 15), pl.ds(0, 4)], got.at[RD])

    with jax.named_scope("xo_wait"):
        arrived(xo.at[pl.ds(0, 3)], got.at[XO])

    with jax.named_scope("outputs"):
        for n in range(NS):
            rn = rall[:, n].astype(F32).reshape(TOK, SW).astype(BF16)
            ob[n] = (xw[n // 2, n % 2].astype(F32) + jnp.dot(t, rn, preferred_element_type=F32)).astype(BF16)
            pltpu.make_async_copy(ob.at[n], out_hbm.at[:, pl.ds(n * SW, SW)], snd.at[OUT]).start()

    with jax.named_scope("drain"):
        for kind, ref in (
            (WZ, wy.at[pl.ds(0, 3), 0]),
            (WD, wy.at[:, pl.ds(0, 2)]),
            (WR, wy.at[:, 0]),
            (WC, wy),
            (XP, xp.at[pl.ds(0, 2)]),
            (XR, xr),
            (XF, xr),
            (XX, xx.at[pl.ds(0, 3)]),
            (DY, dyb.at[:, pl.ds(0, 2)]),
            (RE, dyb.at[:, 0]),
            (RS, sb.at[:, pl.ds(0, 3)]),
            (LF, lf.at[pl.ds(0, 15)]),
            (LA, lall.at[pl.ds(0, 15)]),
            (RT, rsb.at[pl.ds(0, 15)]),
            (RO, rall.at[0, pl.ds(0, 7)]),
            (RC, rall.at[pl.ds(0, 15), pl.ds(0, 4)]),
            (RD, rall.at[pl.ds(0, 15), pl.ds(0, 4)]),
            (XO, xo.at[pl.ds(0, 3)]),
            (NE, mg),
            (OUT, ob),
        ):
            gone(ref, kind)


def step(inputs, out_grads, weight, start_basis, error_buffer):
    vm = pltpu.VMEM
    dma = pltpu.SemaphoreType.DMA
    return pl.pallas_call(
        body,
        out_shape=(
            jax.ShapeDtypeStruct((TOK, D), BF16),
            jax.ShapeDtypeStruct((1, TOK, D), F32),
        ),
        in_specs=[pl.BlockSpec(memory_space=pl.ANY)] * 5,
        out_specs=(pl.BlockSpec(memory_space=pl.ANY),) * 2,
        scratch_shapes=[
            vm((4, 16, TOK, TOK), BF16),
            vm((4, 4, TOK, TOK), BF16),
            vm((4, TOK, TOK), BF16),
            vm((4, TOK, 512), BF16),
            vm((NC, 4, TOK, CW), BF16),
            vm((4, 4, TOK, SW), BF16),
            vm((4, 4, TOK, SW), BF16),
            vm((NC, TOK, CW), F32),
            vm((NC, 8, CW), F32),
            vm((NC, 4, TOK, CW), F32),
            vm((NC, 4, TOK, CW), BF16),
            vm((NC, 4, TOK, CW), BF16),
            vm((NC, 4, TOK, CW), BF16),
            vm((NC, TOK, CW), F32),
            vm((4, 2, TOK, SW), BF16),
            vm((4, 2, TOK, SW), BF16),
            vm((16, 8, TOK), F32),
            vm((16, 8, TOK), F32),
            vm((NS, 8, SW), BF16),
            vm((16, 8, SW), BF16),
            vm((16, NS, 8, SW), BF16),
            vm((NS, TOK, SW), BF16),
            dma((5,)), dma((20,)), dma((20,)), dma((2, 2)), dma((4,)), dma((NC,)), dma((NC,)),
            dma((NC, 4)), dma((NC,)), dma((16,)),
        ],
        compiler_params=pltpu.CompilerParams(
            collective_id=0, has_side_effects=True, vmem_limit_bytes=60 * 1024 * 1024
        ),
    )(inputs, out_grads, weight, start_basis, error_buffer)


def solution(mesh):
    finer = Mesh(mesh.devices.reshape(2, 4, 2, 4, 4), AXES)
    outer = ("zh", "x", "core")
    chip = ("y", "z")
    in_specs = (
        P(outer + chip, None),
        P(outer + chip, None),
        P(chip, None),
        P(chip, None),
        P(outer, chip, None),
    )
    out_specs = (P(outer + chip, None), P(outer, chip, None))
    return jax.shard_map(step, mesh=finer, in_specs=in_specs, out_specs=out_specs, check_vma=False)
```

```python
import jax
import jax.numpy as jnp
from jax import lax
from jax.experimental import pallas as pl
from jax.experimental.pallas import tpu as pltpu
from jax.sharding import Mesh
from jax.sharding import PartitionSpec as P

MESH_ID = pl.DeviceIdType.MESH
AXES = ("zh", "x", "core", "y", "z")
LEARNING_RATE = 0.2
TOK = 128
D = 2048
NC = 16
CW = D // NC
NS = 8
SW = D // NS
LAG = 2
WZ, WD, WR, WC, XP, XR, XF, XX, DY, RE, RS, LF, LA, RT, RO, RC, RD, XO, NE, OUT = range(20)
RO2 = 18
OUTER_PEERS = [(h, i, k) for h in (1, 0) for i in (2, 1, 3, 0) for k in (0, 1) if (h, i, k) != (0, 0, 0)]
CHIP_PEERS = [(j, k) for j in (2, 1, 3, 0) for k in (3, 1, 2, 0) if (j, k) != (0, 0)]
F32 = jnp.float32
BF16 = jnp.bfloat16


def body(
    x_hbm, g_hbm, w_hbm, b_hbm, e_hbm, out_hbm, ne_hbm,
    xx, xp, xr, xgt, dyb, wy, wo, eb, bb, pf, sb, rl, rr, mg, xo, xw, lf, lall, rt, rsb, rall, ob,
    ld, snd, got, xp_r, xr_r, wd_r, dy_r, re_r, rs_r, rz_r, rc_r,
):
    zh, x, core, y, z = (lax.axis_index(a) for a in AXES)
    outer = (zh * 4 + x) * 2 + core
    sl = x * 2 + core
    c = y * 4 + z

    def remote(src, dst, ssem, rsem, dev):
        return pltpu.make_async_remote_copy(
            src_ref=src, dst_ref=dst, send_sem=ssem, recv_sem=rsem,
            device_id=dev, device_id_type=MESH_ID,
        )

    def outer_dev(o):
        return {"zh": (zh + o[0]) % 2, "x": (x + o[1]) % 4, "core": (core + o[2]) % 2}

    def outer_at(o):
        dev = outer_dev(o)
        return (dev["zh"] * 4 + dev["x"]) * 2 + dev["core"]

    def chip_dev(k):
        return {"y": (y + k[0]) % 4, "z": (z + k[1]) % 4}

    def chip_at(k):
        dev = chip_dev(k)
        return dev["y"] * 4 + dev["z"]

    ring = ((y + 1) % 4, (y + 3) % 4)
    y2 = (y + 2) % 4
    near = (3, 1)
    goal = (3 - 3 * (z // 2), 2 - z // 2, z + 1 - 2 * (z % 2), z)
    z_up, z_down = (z + 1) % 4, (z + 3) % 4

    def x_load(q, sem):
        return pltpu.make_async_copy(x_hbm.at[:, pl.ds(pl.multiple_of(q * TOK, TOK), TOK)], xx.at[x, q], ld.at[sem])

    def g_load(n, sem):
        return pltpu.make_async_copy(g_hbm.at[:, pl.ds(n * CW, CW)], dyb.at[n, 0], ld.at[sem])

    for k in range(4):
        x_load(k * 4 + goal[0], 0).start()
    for n in range(2):
        g_load(n, 1).start()

    barrier = pltpu.get_barrier_semaphore()
    for dev in OUTER_PEERS:
        pl.semaphore_signal(barrier, inc=1, device_id=outer_dev(dev), device_id_type=MESH_ID)
    for dev in CHIP_PEERS:
        pl.semaphore_signal(barrier, inc=1, device_id=chip_dev(dev), device_id_type=MESH_ID)

    for g in (1, 2, 3):
        for k in range(4):
            x_load(k * 4 + goal[g], 2).start()
    for n in range(2, NC):
        g_load(n, 3).start()
    w_ld = pltpu.make_async_copy(w_hbm.at[:, pl.ds(pl.multiple_of(sl * SW, SW), SW)], wy.at[z, 0], ld.at[4])
    w_ld.start()

    def arrived(ref, sem):
        remote(ref, ref, snd.at[0], sem, {"core": 1 - core}).wait_recv()

    def gone(ref, kind):
        remote(ref, ref, snd.at[kind], got.at[0], {"core": 1 - core}).wait_send()

    arrived(xx.at[x, pl.ds(0, 4)], ld.at[0])
    arrived(dyb.at[pl.ds(0, 2), 0], ld.at[1])
    with jax.named_scope("entry_barrier"):
        pl.semaphore_wait(barrier, 30)

    def wz_copy(p):
        return remote(wy.at[z, 0], wy.at[z, 0], snd.at[WZ], got.at[WZ], {"z": p})

    def wd_copy(way, j):
        return remote(wy.at[j, 0], wy.at[j, near[way]], snd.at[WD], wd_r.at[j], {"y": ring[way]})

    def wr_copy(j, way):
        return remote(wy.at[j, near[way]], wy.at[j, 2], snd.at[WR], got.at[WR], {"y": ring[way]})

    def wc_copy():
        return remote(wy, wo, snd.at[WC], got.at[WC], {"core": 1 - core})

    def xp_copy(way, g):
        p = ring[way]
        return remote(xx.at[x, p * 4 + goal[g]], xp.at[near[way], g], snd.at[XP], xp_r.at[0, g], {"y": p})

    def xr_copy(g):
        return remote(xx.at[x, y2 * 4 + goal[g]], xr.at[g], snd.at[XR], xr_r.at[g], {"y": ring[g % 2]})

    def far_x():
        return remote(xx.at[x, y2 * 4 + goal[0]], xp.at[2, 0], snd.at[XR], xp_r.at[1, 0], {"y": y2})

    def xf_copy(g):
        return remote(xr.at[g], xp.at[2, g], snd.at[XF], xp_r.at[1, g], {"y": ring[g % 2]})

    def xx_copy(p):
        return remote(xx.at[x], xx.at[x], snd.at[XX], got.at[XX], {"x": p})

    def dy_copy(way, n):
        return remote(dyb.at[n, 0], dyb.at[n, near[way]], snd.at[DY], dy_r.at[n], {"y": ring[way]})

    def relay(n, way):
        return remote(dyb.at[n, near[way]], dyb.at[n, 2], snd.at[RE], re_r.at[n], {"y": ring[way]})

    def direct(n):
        for way in range(2):
            dy_copy(way, n).start()

    def pass_on(n):
        with jax.named_scope("direct_wait"):
            arrived(dyb.at[n, pl.ds(0, 2)], dy_r.at[n])
        for way in range(2):
            @pl.when(n % 2 == way)
            def _():
                relay(n, way).start()

    def send_x(g):
        for way in range(2):
            xp_copy(way, g).start()

    def pass_x(g):
        with jax.named_scope("xr_wait"):
            xr_copy(g).wait_recv()
        xf_copy(g).start()

    def gather_x(g, slots):
        with jax.named_scope("xp_wait"):
            if slots == (1, 3):
                arrived(xr.at[pl.ds(0, 2)], xp_r.at[0, g])
            if slots == (2,):
                arrived(xr.at[0], xp_r.at[1, g])
        for k in slots:
            piece = xp[k, g] if k else xx[x, y * 4 + goal[g]]
            xgt[g, :, pl.ds(k * TOK, TOK)] = piece.T

    def product(n, g):
        return jnp.dot(xgt[g], dyb[n].reshape(4 * TOK, CW), preferred_element_type=F32)

    def send_right(n, d):
        cp = remote(sb.at[n, d], rl.at[n, d], snd.at[RS], rs_r.at[n, d], {"z": z_up})

        @pl.when(z == 0)
        def _():
            sb[n, d] = pf[n, d].astype(BF16)

        @pl.when(z > 0)
        def _():
            with jax.named_scope("right_wait"):
                cp.wait_recv()
            sb[n, d] = (pf[n, d] + rl[n, d].astype(F32)).astype(BF16)

        cp.start()

    def send_left(n, d, h):
        def copy(sem):
            return remote(sb.at[n, d], rr.at[n, d], snd.at[RS], sem, {"z": z_down})


        @pl.when(z == 3)
        def _():
            sb[n, d] = pf[n, d].astype(BF16)

        @pl.when(z < 3)
        def _():
            with jax.named_scope("left_wait"):
                copy(rs_r.at[n, d]).wait_recv()
            sb[n, d] = (pf[n, d] + rr[n, d].astype(F32)).astype(BF16)

        if h > 1:
            copy(rs_r.at[n, d]).start()
        else:
            copy(rz_r.at[n]).start()

    def xo_copy(p):
        return remote(xo.at[p], xw.at[x], snd.at[XO], got.at[XO], {"x": p})

    far_x().start()
    direct(0)
    send_x(0)
    direct(1)
    arrived(xx.at[x, pl.ds(0, 12)], ld.at[2])
    xr_copy(1).start()
    w_ld.wait()
    for i in range(1, 4):
        wz_copy((z + i) % 4).start()
    for i in (1, 3, 2):
        xx_copy((x + i) % 4).start()
    arrived(dyb.at[pl.ds(0, NC - 2), 0], ld.at[3])
    for n in range(NC):
        pltpu.make_async_copy(b_hbm.at[:, pl.ds(n * CW, CW)], bb.at[n], ld.at[5]).start()
        pltpu.make_async_copy(e_hbm.at[0, :, pl.ds(n * CW, CW)], eb.at[n], ld.at[6]).start()
    gather_x(0, (0,))
    pass_on(0)
    direct(2)
    send_x(1)
    direct(3)
    gather_x(0, (1, 3))
    pass_on(1)
    pass_x(1)
    direct(4)
    gather_x(0, (2,))
    with jax.named_scope("relay_wait"):
        relay(0, 0).wait_recv()
    with jax.named_scope("product"):
        pf[0, goal[0]] = product(0, 0)

    @pl.when(z == 0)
    def _():
        send_right(0, 3)

    @pl.when(z == 3)
    def _():
        send_left(0, 0, 3)

    xr_copy(2).start()
    pass_on(2)
    send_x(2)
    direct(5)
    gather_x(1, (0,))

    arrived(bb, ld.at[5])
    arrived(eb, ld.at[6])
    lf[outer] = jnp.zeros((8, TOK), F32)

    @pl.loop(0, NC + 3 * LAG)
    def _(s):
        @pl.when((s >= 1) & (s + 2 < NC))
        def _():
            pass_on(s + 2)

        @pl.when((s >= 1) & (s + 5 < NC))
        def _():
            direct(s + 5)

        for g in (1, 2, 3):
            @pl.when(s == LAG * g)
            def _():
                gather_x(g, (1, 3))
                gather_x(g, (2,))

        @pl.when(s == 1)
        def _():
            with jax.named_scope("wz_wait"):
                arrived(wy.at[pl.ds(0, 3), 0], got.at[WZ])

        @pl.when((s >= 11) & (s < 15))
        def _():
            for way in range(2):
                wd_copy(way, s - 11).start()

        for way in range(2):
            @pl.when((s >= 14) & (s < 18) & (s % 2 == way))
            def _():
                j = s - 14
                with jax.named_scope("wd_wait"):
                    arrived(wy.at[j, pl.ds(0, 2)], wd_r.at[j])
                wr_copy(j, way).start()

        @pl.when(s == NC + 4)
        def _():
            with jax.named_scope("wr_wait"):
                arrived(wy.at[:, 2], got.at[WR])
            wc_copy().start()

        @pl.when((s >= 1) & (s < NC))
        def _():
            with jax.named_scope("relay_wait"):
                relay(s, 0).wait_recv()
            with jax.named_scope("product"):
                pf[s, goal[0]] = product(s, 0)

        for g in (1, 2):
            @pl.when((s >= LAG * g) & (s < NC + LAG * g))
            def _():
                with jax.named_scope("product"):
                    pf[s - LAG * g, goal[g]] = product(s - LAG * g, g)

        for h in (3, 2, 1):
            n = s - LAG * (3 - h)
            ready = (n >= 0) & (n < NC)
            if h == 3:
                ready = ready & (n > 0)

            @pl.when(ready & (z + h < 4))
            def _():
                send_right(n, z + h)

            @pl.when(ready & (z - h >= 0))
            def _():
                send_left(n, z - h, h)

        @pl.when(s == 1)
        def _():
            pass_x(2)
            xr_copy(3).start()
            send_x(3)
            gather_x(2, (0,))

        @pl.when(s == 3)
        def _():
            pass_x(3)
            gather_x(3, (0,))

        @pl.when(s >= 3 * LAG)
        def _():
            n = s - 3 * LAG
            mg[n] = product(n, 3)

            @pl.when(z > 0)
            def _():
                with jax.named_scope("last_wait"):
                    remote(sb.at[n, z], rl.at[n, z], snd.at[RS], rs_r.at[n, z], {"z": z_up}).wait_recv()
                mg[n] = mg[n] + rl[n, z].astype(F32)

            @pl.when(z < 3)
            def _():
                with jax.named_scope("last_wait"):
                    remote(sb.at[n, z], rr.at[n, z], snd.at[RS], rz_r.at[n], {"z": z_down}).wait_recv()
                mg[n] = mg[n] + rr[n, z].astype(F32)

            with jax.named_scope("merge"):
                m = mg[n] * (1.0 / TOK) + eb[n]
                mg[n] = m
                lf[outer] = lf[outer] + lax.dot_general(
                    bb[n], m, (((1,), (1,)), ((), ())), precision=lax.Precision.HIGHEST, preferred_element_type=F32
                )

    def lf_copy(i, own):
        o = OUTER_PEERS[i]
        return remote(lf.at[own], lf.at[own], snd.at[LF], got.at[LF], outer_dev(o))

    for i in range(15):
        lf_copy(i, outer).start()

    with jax.named_scope("xx_wait"):
        arrived(xx.at[pl.ds(0, 3)], got.at[XX])
    with jax.named_scope("wc_wait"):
        wc_copy().wait_recv()
    with jax.named_scope("inputs_weight"):
        for h, half in ((core, wy), (1 - core, wo)):
            acc = jnp.zeros((512, SW), F32)
            for j in range(4):
                left = jnp.concatenate([xx[:, ((y + k) % 4) * 4 + j].reshape(512, TOK) for k in range(4)], axis=1)
                acc = acc + jnp.dot(left, half[j].reshape(512, SW), preferred_element_type=F32)
            xo[:, h] = acc.reshape(4, TOK, SW).astype(BF16)
    xw[x] = xo[x]

    with jax.named_scope("lf_wait"):
        arrived(lf.at[pl.ds(0, 15)], got.at[LF])

    with jax.named_scope("gram_schmidt"):
        v = jnp.sum(lf[...], axis=0) * (1.0 / 16)
        rows = lax.broadcasted_iota(jnp.int32, (8, TOK), 0)
        for k in range(8):
            row = v[k:k + 1]
            dots = jnp.sum(v * row, axis=-1, keepdims=True)
            norm = jnp.sqrt(dots[k:k + 1] + 1.0)
            unit = row / norm
            v = jnp.where(rows > k, v - (dots / norm) * unit, jnp.where(rows == k, unit, v))
        lall[c] = v

    def la_copy(i, own):
        return remote(lall.at[own], lall.at[own], snd.at[LA], got.at[LA], chip_dev(CHIP_PEERS[i]))

    with jax.named_scope("right_product"):
        vh = v.astype(BF16)
        for n in range(NC):
            rt[n // 2, :, pl.ds((n % 2) * CW, CW)] = jnp.dot(
                vh, mg[n].astype(BF16), preferred_element_type=F32
            ).astype(BF16)

    def rt_copy(i, to, own):
        return remote(rt.at[to % 8], rsb.at[own], snd.at[RT], got.at[RT], outer_dev(OUTER_PEERS[i]))

    for i in range(15):
        rt_copy(i, outer_at(OUTER_PEERS[i]), outer).start()

    rsb[outer] = rt[sl]

    with jax.named_scope("rt_wait"):
        arrived(rsb.at[pl.ds(0, 15)], got.at[RT])

    rall[c, sl] = (jnp.sum(rsb[...].astype(F32), axis=0) * (1.0 / 16)).astype(BF16)

    def ro_copy(i, own, sem):
        return remote(rall.at[c, own], rall.at[c, own], snd.at[RO], got.at[sem], outer_dev(OUTER_PEERS[i]))

    for i in range(8, 15):
        hands_on = outer_dev(OUTER_PEERS[i])["core"] == x // 2

        @pl.when(hands_on)
        def _():
            ro_copy(i, sl, RO).start()

        @pl.when(jnp.logical_not(hands_on))
        def _():
            ro_copy(i, sl, RO2).start()
    for i in (1, 3, 2):
        xo_copy((x + i) % 4).start()
    for i in range(15):
        la_copy(i, c).start()

    def half_of(k):
        return pl.ds(k * 4, 4)

    def rc_copy(i, own):
        part = rall.at[own, half_of(core)]
        return remote(part, part, snd.at[RC], rc_r.at[own], chip_dev(CHIP_PEERS[i]))

    def rd_copy(own, k):
        part = rall.at[own, half_of(k)]
        return remote(part, part, snd.at[RD], got.at[RD], {"core": 1 - core})

    def ro_wait(sem, with_own):
        with jax.named_scope("ro_wait"):
            @pl.when(with_own)
            def _():
                arrived(rall.at[c, pl.ds(0, 3)], got.at[sem])

            @pl.when(jnp.logical_not(with_own))
            def _():
                arrived(rall.at[c, pl.ds(0, 4)], got.at[sem])

    ro_wait(RO, x // 2 == core)
    for i in range(15):
        rc_copy(i, c).start()
    ro_wait(RO2, x // 2 != core)

    with jax.named_scope("new_error"):
        vt = v.T
        vt_hi = vt.astype(BF16)
        vt_lo = (vt - vt_hi.astype(F32)).astype(BF16)
        for n in range(NC):
            rn = rall[c, n // 2, :, pl.ds((n % 2) * CW, CW)]
            approx = jnp.dot(vt_hi, rn, preferred_element_type=F32) + jnp.dot(vt_lo, rn, preferred_element_type=F32)
            mg[n] = mg[n] - approx
            pltpu.make_async_copy(mg.at[n], ne_hbm.at[0, :, pl.ds(n * CW, CW)], snd.at[NE]).start()

    with jax.named_scope("la_wait"):
        arrived(lall.at[pl.ds(0, 15)], got.at[LA])

    with jax.named_scope("inputs_left"):
        lmat = lall[...].reshape(TOK, TOK)
        lrow = lax.broadcasted_iota(jnp.int32, (TOK, TOK), 0) // 8
        t = jnp.zeros((TOK, TOK), F32)
        for q in range(4):
            lq = jnp.concatenate(
                [jnp.where(lrow == q * 4 + j, lmat, 0.0).astype(BF16) for j in range(4)], axis=1
            )
            xq = jnp.concatenate([xx[x, q * 4 + j] for j in range(4)], axis=1)
            t = t + lax.dot_general(xq, lq, (((1,), (1,)), ((), ())), preferred_element_type=F32)
        t = (t * (-LEARNING_RATE)).astype(BF16)

    with jax.named_scope("rc_wait"):
        for i in reversed(range(15)):
            p = chip_at(CHIP_PEERS[i])
            rc_copy(i, p).wait_recv()
            rd_copy(p, core).start()
    with jax.named_scope("rd_wait"):
        arrived(rall.at[pl.ds(0, 15), pl.ds(0, 4)], got.at[RD])

    with jax.named_scope("xo_wait"):
        arrived(xo.at[pl.ds(0, 3)], got.at[XO])

    with jax.named_scope("outputs"):
        for n in range(NS):
            rn = rall[:, n].astype(F32).reshape(TOK, SW).astype(BF16)
            ob[n] = (xw[n // 2, n % 2].astype(F32) + jnp.dot(t, rn, preferred_element_type=F32)).astype(BF16)
            pltpu.make_async_copy(ob.at[n], out_hbm.at[:, pl.ds(n * SW, SW)], snd.at[OUT]).start()

    with jax.named_scope("drain"):
        for kind, ref in (
            (WZ, wy.at[pl.ds(0, 3), 0]),
            (WD, wy.at[:, pl.ds(0, 2)]),
            (WR, wy.at[:, 0]),
            (WC, wy),
            (XP, xp.at[pl.ds(0, 2)]),
            (XR, xr),
            (XF, xr.at[pl.ds(0, 3)]),
            (XX, xx.at[pl.ds(0, 3)]),
            (DY, dyb.at[:, pl.ds(0, 2)]),
            (RE, dyb.at[:, 0]),
            (RS, sb.at[:, pl.ds(0, 3)]),
            (LF, lf.at[pl.ds(0, 15)]),
            (LA, lall.at[pl.ds(0, 15)]),
            (RT, rsb.at[pl.ds(0, 15)]),
            (RO, rall.at[0, pl.ds(0, 7)]),
            (RC, rall.at[pl.ds(0, 15), pl.ds(0, 4)]),
            (RD, rall.at[pl.ds(0, 15), pl.ds(0, 4)]),
            (XO, xo.at[pl.ds(0, 3)]),
            (NE, mg),
            (OUT, ob),
        ):
            gone(ref, kind)


def step(inputs, out_grads, weight, start_basis, error_buffer):
    vm = pltpu.VMEM
    dma = pltpu.SemaphoreType.DMA
    return pl.pallas_call(
        body,
        out_shape=(
            jax.ShapeDtypeStruct((TOK, D), BF16),
            jax.ShapeDtypeStruct((1, TOK, D), F32),
        ),
        in_specs=[pl.BlockSpec(memory_space=pl.ANY)] * 5,
        out_specs=(pl.BlockSpec(memory_space=pl.ANY),) * 2,
        scratch_shapes=[
            vm((4, 16, TOK, TOK), BF16),
            vm((4, 4, TOK, TOK), BF16),
            vm((4, TOK, TOK), BF16),
            vm((4, TOK, 512), BF16),
            vm((NC, 4, TOK, CW), BF16),
            vm((4, 4, TOK, SW), BF16),
            vm((4, 4, TOK, SW), BF16),
            vm((NC, TOK, CW), F32),
            vm((NC, 8, CW), F32),
            vm((NC, 4, TOK, CW), F32),
            vm((NC, 4, TOK, CW), BF16),
            vm((NC, 4, TOK, CW), BF16),
            vm((NC, 4, TOK, CW), BF16),
            vm((NC, TOK, CW), F32),
            vm((4, 2, TOK, SW), BF16),
            vm((4, 2, TOK, SW), BF16),
            vm((16, 8, TOK), F32),
            vm((16, 8, TOK), F32),
            vm((NS, 8, SW), BF16),
            vm((16, 8, SW), BF16),
            vm((16, NS, 8, SW), BF16),
            vm((NS, TOK, SW), BF16),
            dma((7,)), dma((20,)), dma((20,)), dma((2, 4)), dma((4,)), dma((4,)), dma((NC,)), dma((NC,)),
            dma((NC, 4)), dma((NC,)), dma((16,)),
        ],
        compiler_params=pltpu.CompilerParams(
            collective_id=0, has_side_effects=True, vmem_limit_bytes=60 * 1024 * 1024
        ),
    )(inputs, out_grads, weight, start_basis, error_buffer)


def solution(mesh):
    finer = Mesh(mesh.devices.reshape(2, 4, 2, 4, 4), AXES)
    outer = ("zh", "x", "core")
    chip = ("y", "z")
    in_specs = (
        P(outer + chip, None),
        P(outer + chip, None),
        P(chip, None),
        P(chip, None),
        P(outer, chip, None),
    )
    out_specs = (P(outer + chip, None), P(outer, chip, None))
    return jax.shard_map(step, mesh=finer, in_specs=in_specs, out_specs=out_specs, check_vma=False)
```

```python
import jax
import jax.numpy as jnp
from jax import lax
from jax.experimental import pallas as pl
from jax.experimental.pallas import tpu as pltpu
from jax.sharding import Mesh
from jax.sharding import PartitionSpec as P

MESH_ID = pl.DeviceIdType.MESH
AXES = ("zh", "x", "core", "y", "z")
LEARNING_RATE = 0.2
TOK = 128
D = 2048
NC = 16
CW = D // NC
NS = 8
SW = D // NS
LAGS = (2, 3)
EARLY = 6
WZ, WD, WR, WC, XP, XR, XF, XX, DY, RE, RS, LF, LA, RT, RO, RC, RD, XO, NE, OUT = range(20)
RO2 = 18
OUTER_PEERS = [(h, i, k) for h in (1, 0) for i in (2, 1, 3, 0) for k in (0, 1) if (h, i, k) != (0, 0, 0)]
CHIP_PEERS = [(j, k) for j in (2, 1, 3, 0) for k in (3, 1, 2, 0) if (j, k) != (0, 0)]
F32 = jnp.float32
BF16 = jnp.bfloat16


def body(
    x_hbm, g_hbm, w_hbm, b_hbm, e_hbm, out_hbm, ne_hbm,
    xx, xp, xr, xgt, dyb, wy, wo, eb, bb, pf, sb, rl, rr, mg, xo, xw, lf, lall, rt, rsb, rall, ob,
    ld, snd, got, xp_r, xr_r, wd_r, dy_r, re_r, rs_r, rz_r, rc_r,
):
    zh, x, core, y, z = (lax.axis_index(a) for a in AXES)
    outer = (zh * 4 + x) * 2 + core
    sl = x * 2 + core
    c = y * 4 + z

    def remote(src, dst, ssem, rsem, dev):
        return pltpu.make_async_remote_copy(
            src_ref=src, dst_ref=dst, send_sem=ssem, recv_sem=rsem,
            device_id=dev, device_id_type=MESH_ID,
        )

    def outer_dev(o):
        return {"zh": (zh + o[0]) % 2, "x": (x + o[1]) % 4, "core": (core + o[2]) % 2}

    def outer_at(o):
        dev = outer_dev(o)
        return (dev["zh"] * 4 + dev["x"]) * 2 + dev["core"]

    def chip_dev(k):
        return {"y": (y + k[0]) % 4, "z": (z + k[1]) % 4}

    def chip_at(k):
        dev = chip_dev(k)
        return dev["y"] * 4 + dev["z"]

    ring = ((y + 1) % 4, (y + 3) % 4)
    y2 = (y + 2) % 4
    near = (3, 1)
    goal = (3 - 3 * (z // 2), 2 - z // 2, z + 1 - 2 * (z % 2), z)
    z_up, z_down = (z + 1) % 4, (z + 3) % 4

    def x_load(q, sem):
        return pltpu.make_async_copy(x_hbm.at[:, pl.ds(pl.multiple_of(q * TOK, TOK), TOK)], xx.at[x, q], ld.at[sem])

    def g_load(n, sem):
        return pltpu.make_async_copy(g_hbm.at[:, pl.ds(n * CW, CW)], dyb.at[n, 0], ld.at[sem])

    for k in range(4):
        x_load(k * 4 + goal[0], 0).start()
    for n in range(2):
        g_load(n, 1).start()

    barrier = pltpu.get_barrier_semaphore()
    for dev in OUTER_PEERS:
        pl.semaphore_signal(barrier, inc=1, device_id=outer_dev(dev), device_id_type=MESH_ID)
    for dev in CHIP_PEERS:
        pl.semaphore_signal(barrier, inc=1, device_id=chip_dev(dev), device_id_type=MESH_ID)

    for g in (1, 2, 3):
        for k in range(4):
            x_load(k * 4 + goal[g], 2).start()
    for n in range(2, NC):
        g_load(n, 3).start()
    w_ld = pltpu.make_async_copy(w_hbm.at[:, pl.ds(pl.multiple_of(sl * SW, SW), SW)], wy.at[z, 0], ld.at[4])
    w_ld.start()

    def arrived(ref, sem):
        remote(ref, ref, snd.at[0], sem, {"core": 1 - core}).wait_recv()

    def gone(ref, kind):
        remote(ref, ref, snd.at[kind], got.at[0], {"core": 1 - core}).wait_send()

    arrived(xx.at[x, pl.ds(0, 4)], ld.at[0])
    arrived(dyb.at[pl.ds(0, 2), 0], ld.at[1])
    with jax.named_scope("entry_barrier"):
        pl.semaphore_wait(barrier, 30)

    def wz_copy(p):
        return remote(wy.at[z, 0], wy.at[z, 0], snd.at[WZ], got.at[WZ], {"z": p})

    def wd_copy(way, j):
        return remote(wy.at[j, 0], wy.at[j, near[way]], snd.at[WD], wd_r.at[j], {"y": ring[way]})

    def wr_copy(j, way):
        return remote(wy.at[j, near[way]], wy.at[j, 2], snd.at[WR], got.at[WR], {"y": ring[way]})

    def wc_copy():
        return remote(wy, wo, snd.at[WC], got.at[WC], {"core": 1 - core})

    def xp_copy(way, g):
        p = ring[way]
        return remote(xx.at[x, p * 4 + goal[g]], xp.at[near[way], g], snd.at[XP], xp_r.at[0, g], {"y": p})

    def xr_copy(g):
        return remote(xx.at[x, y2 * 4 + goal[g]], xr.at[g], snd.at[XR], xr_r.at[g], {"y": ring[g % 2]})

    def far_x():
        return remote(xx.at[x, y2 * 4 + goal[0]], xp.at[2, 0], snd.at[XR], xp_r.at[1, 0], {"y": y2})

    def xf_copy(g):
        return remote(xr.at[g], xp.at[2, g], snd.at[XF], xp_r.at[1, g], {"y": ring[g % 2]})

    def xx_copy(p):
        return remote(xx.at[x], xx.at[x], snd.at[XX], got.at[XX], {"x": p})

    def dy_copy(way, n):
        return remote(dyb.at[n, 0], dyb.at[n, near[way]], snd.at[DY], dy_r.at[n], {"y": ring[way]})

    def relay(n, way):
        return remote(dyb.at[n, near[way]], dyb.at[n, 2], snd.at[RE], re_r.at[n], {"y": ring[way]})

    def direct(n):
        for way in range(2):
            dy_copy(way, n).start()

    def pass_on(n):
        with jax.named_scope("direct_wait"):
            arrived(dyb.at[n, pl.ds(0, 2)], dy_r.at[n])
        for way in range(2):
            @pl.when(n % 2 == way)
            def _():
                relay(n, way).start()

    def send_x(g):
        for way in range(2):
            xp_copy(way, g).start()

    def pass_x(g):
        with jax.named_scope("xr_wait"):
            xr_copy(g).wait_recv()
        xf_copy(g).start()

    def gather_x(g, slots):
        with jax.named_scope("xp_wait"):
            if slots == (1, 3):
                arrived(xr.at[pl.ds(0, 2)], xp_r.at[0, g])
            if slots == (2,):
                arrived(xr.at[0], xp_r.at[1, g])
        for k in slots:
            piece = xp[k, g] if k else xx[x, y * 4 + goal[g]]
            xgt[g, :, pl.ds(k * TOK, TOK)] = piece.T

    def product(n, g):
        return jnp.dot(xgt[g], dyb[n].reshape(4 * TOK, CW), preferred_element_type=F32)

    def send_right(n, d):
        cp = remote(sb.at[n, d], rl.at[n, d], snd.at[RS], rs_r.at[n, d], {"z": z_up})

        @pl.when(z == 0)
        def _():
            sb[n, d] = pf[n, d].astype(BF16)

        @pl.when(z > 0)
        def _():
            with jax.named_scope("right_wait"):
                cp.wait_recv()
            sb[n, d] = (pf[n, d] + rl[n, d].astype(F32)).astype(BF16)

        cp.start()

    def send_left(n, d, h):
        def copy(sem):
            return remote(sb.at[n, d], rr.at[n, d], snd.at[RS], sem, {"z": z_down})


        @pl.when(z == 3)
        def _():
            sb[n, d] = pf[n, d].astype(BF16)

        @pl.when(z < 3)
        def _():
            with jax.named_scope("left_wait"):
                copy(rs_r.at[n, d]).wait_recv()
            sb[n, d] = (pf[n, d] + rr[n, d].astype(F32)).astype(BF16)

        if h > 1:
            copy(rs_r.at[n, d]).start()
        else:
            copy(rz_r.at[n]).start()

    def xo_copy(p):
        return remote(xo.at[p], xw.at[x], snd.at[XO], got.at[XO], {"x": p})

    far_x().start()
    direct(0)
    send_x(0)
    direct(1)
    arrived(xx.at[x, pl.ds(0, 12)], ld.at[2])
    xr_copy(1).start()
    w_ld.wait()
    for i in range(1, 4):
        wz_copy((z + i) % 4).start()
    for i in (1, 3, 2):
        xx_copy((x + i) % 4).start()
    arrived(dyb.at[pl.ds(0, NC - 2), 0], ld.at[3])
    for n in range(NC):
        pltpu.make_async_copy(b_hbm.at[:, pl.ds(n * CW, CW)], bb.at[n], ld.at[5]).start()
        pltpu.make_async_copy(e_hbm.at[0, :, pl.ds(n * CW, CW)], eb.at[n], ld.at[6]).start()
    gather_x(0, (0,))
    pass_on(0)
    direct(2)
    send_x(1)
    direct(3)
    gather_x(0, (1, 3))
    pass_on(1)
    pass_x(1)
    direct(4)
    gather_x(0, (2,))
    with jax.named_scope("relay_wait"):
        relay(0, 0).wait_recv()
    with jax.named_scope("product"):
        pf[0, goal[0]] = product(0, 0)

    @pl.when(z == 0)
    def _():
        send_right(0, 3)

    @pl.when(z == 3)
    def _():
        send_left(0, 0, 3)

    xr_copy(2).start()
    pass_on(2)
    send_x(2)
    direct(5)
    gather_x(1, (0,))

    arrived(bb, ld.at[5])
    arrived(eb, ld.at[6])
    lf[outer] = jnp.zeros((8, TOK), F32)

    @pl.loop(0, NC + 3 * LAGS[1])
    def _(s):
        @pl.when((s >= 1) & (s + 2 < NC))
        def _():
            pass_on(s + 2)

        @pl.when((s >= 1) & (s + 5 < NC))
        def _():
            direct(s + 5)

        for g in (1, 2, 3):
            @pl.when(s == LAGS[0] * g)
            def _():
                gather_x(g, (1, 3))
                gather_x(g, (2,))

        @pl.when(s == 1)
        def _():
            with jax.named_scope("wz_wait"):
                arrived(wy.at[pl.ds(0, 3), 0], got.at[WZ])

        @pl.when((s >= 11) & (s < 15))
        def _():
            for way in range(2):
                wd_copy(way, s - 11).start()

        for way in range(2):
            @pl.when((s >= 14) & (s < 18) & (s % 2 == way))
            def _():
                j = s - 14
                with jax.named_scope("wd_wait"):
                    arrived(wy.at[j, pl.ds(0, 2)], wd_r.at[j])
                wr_copy(j, way).start()

        @pl.when(s == NC + 4)
        def _():
            with jax.named_scope("wr_wait"):
                arrived(wy.at[:, 2], got.at[WR])
            wc_copy().start()

        @pl.when((s >= 1) & (s < NC))
        def _():
            with jax.named_scope("relay_wait"):
                relay(s, 0).wait_recv()
            with jax.named_scope("product"):
                pf[s, goal[0]] = product(s, 0)

        def turn(k):
            first, later = s - LAGS[0] * k, s - LAGS[1] * k
            n = jnp.where(first < EARLY, first, later)
            return n, (n >= 0) & (n < NC) & ((first < EARLY) | (later >= EARLY))

        for g in (1, 2):
            n, ready = turn(g)

            @pl.when(ready)
            def _():
                with jax.named_scope("product"):
                    pf[n, goal[g]] = product(n, g)

        for h in (3, 2, 1):
            n, ready = turn(3 - h)
            if h == 3:
                ready = ready & (n > 0)

            @pl.when(ready & (z + h < 4))
            def _():
                send_right(n, z + h)

            @pl.when(ready & (z - h >= 0))
            def _():
                send_left(n, z - h, h)

        @pl.when(s == 1)
        def _():
            pass_x(2)
            gather_x(2, (0,))

        @pl.when(s == 2)
        def _():
            xr_copy(3).start()

        @pl.when(s == 3)
        def _():
            send_x(3)
            gather_x(3, (0,))

        @pl.when(s == 4)
        def _():
            pass_x(3)

        last, ready = turn(3)

        @pl.when(ready)
        def _():
            n = last
            mg[n] = product(n, 3)

            @pl.when(z > 0)
            def _():
                with jax.named_scope("last_wait"):
                    remote(sb.at[n, z], rl.at[n, z], snd.at[RS], rs_r.at[n, z], {"z": z_up}).wait_recv()
                mg[n] = mg[n] + rl[n, z].astype(F32)

            @pl.when(z < 3)
            def _():
                with jax.named_scope("last_wait"):
                    remote(sb.at[n, z], rr.at[n, z], snd.at[RS], rz_r.at[n], {"z": z_down}).wait_recv()
                mg[n] = mg[n] + rr[n, z].astype(F32)

            with jax.named_scope("merge"):
                m = mg[n] * (1.0 / TOK) + eb[n]
                mg[n] = m
                lf[outer] = lf[outer] + lax.dot_general(
                    bb[n], m, (((1,), (1,)), ((), ())), precision=lax.Precision.HIGHEST, preferred_element_type=F32
                )

    def lf_copy(i, own):
        o = OUTER_PEERS[i]
        return remote(lf.at[own], lf.at[own], snd.at[LF], got.at[LF], outer_dev(o))

    for i in range(15):
        lf_copy(i, outer).start()

    with jax.named_scope("xx_wait"):
        arrived(xx.at[pl.ds(0, 3)], got.at[XX])
    with jax.named_scope("wc_wait"):
        wc_copy().wait_recv()
    with jax.named_scope("inputs_weight"):
        for h, half in ((core, wy), (1 - core, wo)):
            acc = jnp.zeros((512, SW), F32)
            for j in range(4):
                left = jnp.concatenate([xx[:, ((y + k) % 4) * 4 + j].reshape(512, TOK) for k in range(4)], axis=1)
                acc = acc + jnp.dot(left, half[j].reshape(512, SW), preferred_element_type=F32)
            xo[:, h] = acc.reshape(4, TOK, SW).astype(BF16)
    xw[x] = xo[x]

    with jax.named_scope("lf_wait"):
        arrived(lf.at[pl.ds(0, 15)], got.at[LF])

    with jax.named_scope("gram_schmidt"):
        v = jnp.sum(lf[...], axis=0) * (1.0 / 16)
        rows = lax.broadcasted_iota(jnp.int32, (8, TOK), 0)
        for k in range(8):
            row = v[k:k + 1]
            dots = jnp.sum(v * row, axis=-1, keepdims=True)
            norm = jnp.sqrt(dots[k:k + 1] + 1.0)
            unit = row / norm
            v = jnp.where(rows > k, v - (dots / norm) * unit, jnp.where(rows == k, unit, v))
        lall[c] = v

    def la_copy(i, own):
        return remote(lall.at[own], lall.at[own], snd.at[LA], got.at[LA], chip_dev(CHIP_PEERS[i]))

    with jax.named_scope("right_product"):
        vh = v.astype(BF16)
        for n in range(NC):
            rt[n // 2, :, pl.ds((n % 2) * CW, CW)] = jnp.dot(
                vh, mg[n].astype(BF16), preferred_element_type=F32
            ).astype(BF16)

    def rt_copy(i, to, own):
        return remote(rt.at[to % 8], rsb.at[own], snd.at[RT], got.at[RT], outer_dev(OUTER_PEERS[i]))

    for i in range(15):
        rt_copy(i, outer_at(OUTER_PEERS[i]), outer).start()

    rsb[outer] = rt[sl]

    with jax.named_scope("rt_wait"):
        arrived(rsb.at[pl.ds(0, 15)], got.at[RT])

    rall[c, sl] = (jnp.sum(rsb[...].astype(F32), axis=0) * (1.0 / 16)).astype(BF16)

    def ro_copy(i, own, sem):
        return remote(rall.at[c, own], rall.at[c, own], snd.at[RO], got.at[sem], outer_dev(OUTER_PEERS[i]))

    for i in range(8, 15):
        hands_on = outer_dev(OUTER_PEERS[i])["core"] == x // 2

        @pl.when(hands_on)
        def _():
            ro_copy(i, sl, RO).start()

        @pl.when(jnp.logical_not(hands_on))
        def _():
            ro_copy(i, sl, RO2).start()
    for i in (1, 3, 2):
        xo_copy((x + i) % 4).start()
    for i in range(15):
        la_copy(i, c).start()

    def half_of(k):
        return pl.ds(k * 4, 4)

    def rc_copy(i, own):
        part = rall.at[own, half_of(core)]
        return remote(part, part, snd.at[RC], rc_r.at[own], chip_dev(CHIP_PEERS[i]))

    def rd_copy(own, k):
        part = rall.at[own, half_of(k)]
        return remote(part, part, snd.at[RD], got.at[RD], {"core": 1 - core})

    def ro_wait(sem, with_own):
        with jax.named_scope("ro_wait"):
            @pl.when(with_own)
            def _():
                arrived(rall.at[c, pl.ds(0, 3)], got.at[sem])

            @pl.when(jnp.logical_not(with_own))
            def _():
                arrived(rall.at[c, pl.ds(0, 4)], got.at[sem])

    ro_wait(RO, x // 2 == core)
    for i in range(15):
        rc_copy(i, c).start()
    ro_wait(RO2, x // 2 != core)

    with jax.named_scope("new_error"):
        vt = v.T
        vt_hi = vt.astype(BF16)
        vt_lo = (vt - vt_hi.astype(F32)).astype(BF16)
        for n in range(NC):
            rn = rall[c, n // 2, :, pl.ds((n % 2) * CW, CW)]
            approx = jnp.dot(vt_hi, rn, preferred_element_type=F32) + jnp.dot(vt_lo, rn, preferred_element_type=F32)
            mg[n] = mg[n] - approx
            pltpu.make_async_copy(mg.at[n], ne_hbm.at[0, :, pl.ds(n * CW, CW)], snd.at[NE]).start()

    with jax.named_scope("la_wait"):
        arrived(lall.at[pl.ds(0, 15)], got.at[LA])

    with jax.named_scope("inputs_left"):
        lmat = lall[...].reshape(TOK, TOK)
        lrow = lax.broadcasted_iota(jnp.int32, (TOK, TOK), 0) // 8
        t = jnp.zeros((TOK, TOK), F32)
        for q in range(4):
            lq = jnp.concatenate(
                [jnp.where(lrow == q * 4 + j, lmat, 0.0).astype(BF16) for j in range(4)], axis=1
            )
            xq = jnp.concatenate([xx[x, q * 4 + j] for j in range(4)], axis=1)
            t = t + lax.dot_general(xq, lq, (((1,), (1,)), ((), ())), preferred_element_type=F32)
        t = (t * (-LEARNING_RATE)).astype(BF16)

    with jax.named_scope("rc_wait"):
        for i in reversed(range(15)):
            p = chip_at(CHIP_PEERS[i])
            rc_copy(i, p).wait_recv()
            rd_copy(p, core).start()
    with jax.named_scope("xo_wait"):
        arrived(xo.at[pl.ds(0, 3)], got.at[XO])

    def finish(first):
        for k in range(4):
            n = first + k
            rn = rall[:, n].astype(F32).reshape(TOK, SW).astype(BF16)
            ob[n] = (xw[n // 2, n % 2].astype(F32) + jnp.dot(t, rn, preferred_element_type=F32)).astype(BF16)
            columns = pl.ds(pl.multiple_of(n * SW, SW), SW)
            pltpu.make_async_copy(ob.at[n], out_hbm.at[:, columns], snd.at[OUT]).start()

    with jax.named_scope("outputs"):
        finish(core * 4)
    with jax.named_scope("rd_wait"):
        arrived(rall.at[pl.ds(0, 15), pl.ds(0, 4)], got.at[RD])
    with jax.named_scope("outputs"):
        finish(4 - core * 4)

    with jax.named_scope("drain"):
        for kind, ref in (
            (WZ, wy.at[pl.ds(0, 3), 0]),
            (WD, wy.at[:, pl.ds(0, 2)]),
            (WR, wy.at[:, 0]),
            (WC, wy),
            (XP, xp.at[pl.ds(0, 2)]),
            (XR, xr),
            (XF, xr.at[pl.ds(0, 3)]),
            (XX, xx.at[pl.ds(0, 3)]),
            (DY, dyb.at[:, pl.ds(0, 2)]),
            (RE, dyb.at[:, 0]),
            (RS, sb.at[:, pl.ds(0, 3)]),
            (LF, lf.at[pl.ds(0, 15)]),
            (LA, lall.at[pl.ds(0, 15)]),
            (RT, rsb.at[pl.ds(0, 15)]),
            (RO, rall.at[0, pl.ds(0, 7)]),
            (RC, rall.at[pl.ds(0, 15), pl.ds(0, 4)]),
            (RD, rall.at[pl.ds(0, 15), pl.ds(0, 4)]),
            (XO, xo.at[pl.ds(0, 3)]),
            (NE, mg),
            (OUT, ob),
        ):
            gone(ref, kind)


def step(inputs, out_grads, weight, start_basis, error_buffer):
    vm = pltpu.VMEM
    dma = pltpu.SemaphoreType.DMA
    return pl.pallas_call(
        body,
        out_shape=(
            jax.ShapeDtypeStruct((TOK, D), BF16),
            jax.ShapeDtypeStruct((1, TOK, D), F32),
        ),
        in_specs=[pl.BlockSpec(memory_space=pl.ANY)] * 5,
        out_specs=(pl.BlockSpec(memory_space=pl.ANY),) * 2,
        scratch_shapes=[
            vm((4, 16, TOK, TOK), BF16),
            vm((4, 4, TOK, TOK), BF16),
            vm((4, TOK, TOK), BF16),
            vm((4, TOK, 512), BF16),
            vm((NC, 4, TOK, CW), BF16),
            vm((4, 4, TOK, SW), BF16),
            vm((4, 4, TOK, SW), BF16),
            vm((NC, TOK, CW), F32),
            vm((NC, 8, CW), F32),
            vm((NC, 4, TOK, CW), F32),
            vm((NC, 4, TOK, CW), BF16),
            vm((NC, 4, TOK, CW), BF16),
            vm((NC, 4, TOK, CW), BF16),
            vm((NC, TOK, CW), F32),
            vm((4, 2, TOK, SW), BF16),
            vm((4, 2, TOK, SW), BF16),
            vm((16, 8, TOK), F32),
            vm((16, 8, TOK), F32),
            vm((NS, 8, SW), BF16),
            vm((16, 8, SW), BF16),
            vm((16, NS, 8, SW), BF16),
            vm((NS, TOK, SW), BF16),
            dma((7,)), dma((20,)), dma((20,)), dma((2, 4)), dma((4,)), dma((4,)), dma((NC,)), dma((NC,)),
            dma((NC, 4)), dma((NC,)), dma((16,)),
        ],
        compiler_params=pltpu.CompilerParams(
            collective_id=0, has_side_effects=True, vmem_limit_bytes=60 * 1024 * 1024
        ),
    )(inputs, out_grads, weight, start_basis, error_buffer)


def solution(mesh):
    finer = Mesh(mesh.devices.reshape(2, 4, 2, 4, 4), AXES)
    outer = ("zh", "x", "core")
    chip = ("y", "z")
    in_specs = (
        P(outer + chip, None),
        P(outer + chip, None),
        P(chip, None),
        P(chip, None),
        P(outer, chip, None),
    )
    out_specs = (P(outer + chip, None), P(outer, chip, None))
    return jax.shard_map(step, mesh=finer, in_specs=in_specs, out_specs=out_specs, check_vma=False)
```

```python
import jax
import jax.numpy as jnp
from jax import lax
from jax.experimental import pallas as pl
from jax.experimental.pallas import tpu as pltpu
from jax.sharding import Mesh
from jax.sharding import PartitionSpec as P

MESH_ID = pl.DeviceIdType.MESH
AXES = ("zh", "x", "core", "y", "z")
LEARNING_RATE = 0.2
TOK = 128
D = 2048
NC = 16
CW = D // NC
NS = 8
SW = D // NS
LAGS = (2, 3)
EARLY = 6
WZ, WD, WR, WC, XP, XR, XF, XX, DY, RE, RS, LF, LA, RT, RO, RC, RD, XO, NE, OUT = range(20)
RO2 = 18
OUTER_PEERS = [(h, i, k) for h in (1, 0) for i in (2, 1, 3, 0) for k in (0, 1) if (h, i, k) != (0, 0, 0)]
CHIP_PEERS = [(j, k) for j in (2, 1, 3, 0) for k in (3, 1, 2, 0) if (j, k) != (0, 0)]
F32 = jnp.float32
BF16 = jnp.bfloat16


def body(
    x_hbm, g_hbm, w_hbm, b_hbm, e_hbm, out_hbm, ne_hbm,
    xx, xp, xr, xgt, dyb, wy, wo, eb, bb, pf, sb, rl, rr, mg, xo, xw, lf, lall, rt, rsb, rall, ob,
    ld, snd, got, xp_r, xr_r, wd_r, dy_r, re_r, rs_r, rz_r, rc_r,
):
    zh, x, core, y, z = (lax.axis_index(a) for a in AXES)
    outer = (zh * 4 + x) * 2 + core
    sl = x * 2 + core
    c = y * 4 + z

    def remote(src, dst, ssem, rsem, dev):
        return pltpu.make_async_remote_copy(
            src_ref=src, dst_ref=dst, send_sem=ssem, recv_sem=rsem,
            device_id=dev, device_id_type=MESH_ID,
        )

    def outer_dev(o):
        return {"zh": (zh + o[0]) % 2, "x": (x + o[1]) % 4, "core": (core + o[2]) % 2}

    def outer_at(o):
        dev = outer_dev(o)
        return (dev["zh"] * 4 + dev["x"]) * 2 + dev["core"]

    def chip_dev(k):
        return {"y": (y + k[0]) % 4, "z": (z + k[1]) % 4}

    def chip_at(k):
        dev = chip_dev(k)
        return dev["y"] * 4 + dev["z"]

    ring = ((y + 1) % 4, (y + 3) % 4)
    y2 = (y + 2) % 4
    near = (3, 1)
    goal = (3 - 3 * (z // 2), 2 - z // 2, z + 1 - 2 * (z % 2), z)
    z_up, z_down = (z + 1) % 4, (z + 3) % 4

    def x_load(q, sem):
        return pltpu.make_async_copy(x_hbm.at[:, pl.ds(pl.multiple_of(q * TOK, TOK), TOK)], xx.at[x, q], ld.at[sem])

    def g_load(n, sem):
        return pltpu.make_async_copy(g_hbm.at[:, pl.ds(n * CW, CW)], dyb.at[n, 0], ld.at[sem])

    for k in range(4):
        x_load(k * 4 + goal[0], 0).start()
    for n in range(2):
        g_load(n, 1).start()

    barrier = pltpu.get_barrier_semaphore()
    for dev in OUTER_PEERS:
        pl.semaphore_signal(barrier, inc=1, device_id=outer_dev(dev), device_id_type=MESH_ID)
    for dev in CHIP_PEERS:
        pl.semaphore_signal(barrier, inc=1, device_id=chip_dev(dev), device_id_type=MESH_ID)

    for g in (1, 2, 3):
        for k in range(4):
            x_load(k * 4 + goal[g], 2).start()
    for n in range(2, NC):
        g_load(n, 3).start()
    w_ld = pltpu.make_async_copy(w_hbm.at[:, pl.ds(pl.multiple_of(sl * SW, SW), SW)], wy.at[z, 0], ld.at[4])
    w_ld.start()

    def arrived(ref, sem):
        remote(ref, ref, snd.at[0], sem, {"core": 1 - core}).wait_recv()

    def gone(ref, kind):
        remote(ref, ref, snd.at[kind], got.at[0], {"core": 1 - core}).wait_send()

    arrived(xx.at[x, pl.ds(0, 4)], ld.at[0])
    arrived(dyb.at[pl.ds(0, 2), 0], ld.at[1])
    with jax.named_scope("entry_barrier"):
        pl.semaphore_wait(barrier, 30)

    def wz_copy(p):
        return remote(wy.at[z, 0], wy.at[z, 0], snd.at[WZ], got.at[WZ], {"z": p})

    def wd_copy(way, j):
        return remote(wy.at[j, 0], wy.at[j, near[way]], snd.at[WD], wd_r.at[j], {"y": ring[way]})

    def wr_copy(j, way):
        return remote(wy.at[j, near[way]], wy.at[j, 2], snd.at[WR], got.at[WR], {"y": ring[way]})

    def wc_copy():
        return remote(wy, wo, snd.at[WC], got.at[WC], {"core": 1 - core})

    def xp_copy(way, g):
        p = ring[way]
        return remote(xx.at[x, p * 4 + goal[g]], xp.at[near[way], g], snd.at[XP], xp_r.at[0, g], {"y": p})

    def xr_copy(g):
        return remote(xx.at[x, y2 * 4 + goal[g]], xr.at[g], snd.at[XR], xr_r.at[g], {"y": ring[g % 2]})

    def far_x():
        return remote(xx.at[x, y2 * 4 + goal[0]], xp.at[2, 0], snd.at[XR], xp_r.at[1, 0], {"y": y2})

    def xf_copy(g):
        return remote(xr.at[g], xp.at[2, g], snd.at[XF], xp_r.at[1, g], {"y": ring[g % 2]})

    def xx_copy(p):
        return remote(xx.at[x], xx.at[x], snd.at[XX], got.at[XX], {"x": p})

    def dy_copy(way, n):
        return remote(dyb.at[n, 0], dyb.at[n, near[way]], snd.at[DY], dy_r.at[n], {"y": ring[way]})

    def relay(n, way):
        return remote(dyb.at[n, near[way]], dyb.at[n, 2], snd.at[RE], re_r.at[n], {"y": ring[way]})

    def direct(n):
        for way in range(2):
            dy_copy(way, n).start()

    def pass_on(n):
        with jax.named_scope("direct_wait"):
            arrived(dyb.at[n, pl.ds(0, 2)], dy_r.at[n])
        for way in range(2):
            @pl.when(n % 2 == way)
            def _():
                relay(n, way).start()

    def send_x(g):
        for way in range(2):
            xp_copy(way, g).start()

    def pass_x(g):
        with jax.named_scope("xr_wait"):
            xr_copy(g).wait_recv()
        xf_copy(g).start()

    def gather_x(g, slots):
        with jax.named_scope("xp_wait"):
            if slots == (1, 3):
                arrived(xr.at[pl.ds(0, 2)], xp_r.at[0, g])
            if slots == (2,):
                arrived(xr.at[0], xp_r.at[1, g])
        for k in slots:
            piece = xp[k, g] if k else xx[x, y * 4 + goal[g]]
            xgt[g, :, pl.ds(k * TOK, TOK)] = piece.T

    def product(n, g):
        return jnp.dot(xgt[g], dyb[n].reshape(4 * TOK, CW), preferred_element_type=F32)

    def send_right(n, d):
        cp = remote(sb.at[n, d], rl.at[n, d], snd.at[RS], rs_r.at[n, d], {"z": z_up})

        @pl.when(z == 0)
        def _():
            sb[n, d] = pf[n, d].astype(BF16)

        @pl.when(z > 0)
        def _():
            with jax.named_scope("right_wait"):
                cp.wait_recv()
            sb[n, d] = (pf[n, d] + rl[n, d].astype(F32)).astype(BF16)

        cp.start()

    def send_left(n, d, h):
        def copy(sem):
            return remote(sb.at[n, d], rr.at[n, d], snd.at[RS], sem, {"z": z_down})


        @pl.when(z == 3)
        def _():
            sb[n, d] = pf[n, d].astype(BF16)

        @pl.when(z < 3)
        def _():
            with jax.named_scope("left_wait"):
                copy(rs_r.at[n, d]).wait_recv()
            sb[n, d] = (pf[n, d] + rr[n, d].astype(F32)).astype(BF16)

        if h > 1:
            copy(rs_r.at[n, d]).start()
        else:
            copy(rz_r.at[n]).start()

    def xo_copy(p):
        return remote(xo.at[p], xw.at[x], snd.at[XO], got.at[XO], {"x": p})

    far_x().start()
    direct(0)
    send_x(0)
    direct(1)
    arrived(xx.at[x, pl.ds(0, 12)], ld.at[2])
    xr_copy(1).start()
    w_ld.wait()
    for i in range(1, 4):
        wz_copy((z + i) % 4).start()
    for i in (1, 3, 2):
        xx_copy((x + i) % 4).start()
    arrived(dyb.at[pl.ds(0, NC - 2), 0], ld.at[3])
    for n in range(NC):
        pltpu.make_async_copy(b_hbm.at[:, pl.ds(n * CW, CW)], bb.at[n], ld.at[5]).start()
        pltpu.make_async_copy(e_hbm.at[0, :, pl.ds(n * CW, CW)], eb.at[n], ld.at[6]).start()
    gather_x(0, (0,))
    pass_on(0)
    direct(2)
    send_x(1)
    direct(3)
    gather_x(0, (1, 3))
    pass_on(1)
    pass_x(1)
    direct(4)
    gather_x(0, (2,))
    with jax.named_scope("relay_wait"):
        relay(0, 0).wait_recv()
    with jax.named_scope("product"):
        pf[0, goal[0]] = product(0, 0)

    @pl.when(z == 0)
    def _():
        send_right(0, 3)

    @pl.when(z == 3)
    def _():
        send_left(0, 0, 3)

    xr_copy(2).start()
    pass_on(2)
    send_x(2)
    direct(5)
    gather_x(1, (0,))

    arrived(bb, ld.at[5])
    arrived(eb, ld.at[6])
    lf[outer] = jnp.zeros((8, TOK), F32)

    @pl.loop(0, NC + 3 * LAGS[1])
    def _(s):
        @pl.when((s >= 1) & (s + 2 < NC))
        def _():
            pass_on(s + 2)

        @pl.when((s >= 1) & (s + 5 < NC))
        def _():
            direct(s + 5)

        for g in (1, 2, 3):
            @pl.when(s == LAGS[0] * g)
            def _():
                gather_x(g, (1, 3))
                gather_x(g, (2,))

        @pl.when(s == 1)
        def _():
            with jax.named_scope("wz_wait"):
                arrived(wy.at[pl.ds(0, 3), 0], got.at[WZ])

        @pl.when((s >= 11) & (s < 15))
        def _():
            for way in range(2):
                wd_copy(way, s - 11).start()

        for way in range(2):
            @pl.when((s >= 14) & (s < 18) & (s % 2 == way))
            def _():
                j = s - 14
                with jax.named_scope("wd_wait"):
                    arrived(wy.at[j, pl.ds(0, 2)], wd_r.at[j])
                wr_copy(j, way).start()

        @pl.when(s == NC + 4)
        def _():
            with jax.named_scope("wr_wait"):
                arrived(wy.at[:, 2], got.at[WR])
            wc_copy().start()

        @pl.when((s >= 1) & (s < NC))
        def _():
            with jax.named_scope("relay_wait"):
                relay(s, 0).wait_recv()
            with jax.named_scope("product"):
                pf[s, goal[0]] = product(s, 0)

        def turn(k):
            first, later = s - LAGS[0] * k, s - LAGS[1] * k
            n = jnp.where(first < EARLY, first, later)
            return n, (n >= 0) & (n < NC) & ((first < EARLY) | (later >= EARLY))

        for g in (1, 2):
            n, ready = turn(g)

            @pl.when(ready)
            def _():
                with jax.named_scope("product"):
                    pf[n, goal[g]] = product(n, g)

        for h in (3, 2, 1):
            n, ready = turn(3 - h)
            if h == 3:
                ready = ready & (n > 0)

            @pl.when(ready & (z + h < 4))
            def _():
                send_right(n, z + h)

            @pl.when(ready & (z - h >= 0))
            def _():
                send_left(n, z - h, h)

        @pl.when(s == 1)
        def _():
            pass_x(2)
            gather_x(2, (0,))

        @pl.when(s == 2)
        def _():
            xr_copy(3).start()

        @pl.when(s == 3)
        def _():
            send_x(3)
            gather_x(3, (0,))

        @pl.when(s == 4)
        def _():
            pass_x(3)

        last, ready = turn(3)

        @pl.when(ready)
        def _():
            n = last
            mg[n] = product(n, 3)

            @pl.when(z > 0)
            def _():
                with jax.named_scope("last_wait"):
                    remote(sb.at[n, z], rl.at[n, z], snd.at[RS], rs_r.at[n, z], {"z": z_up}).wait_recv()
                mg[n] = mg[n] + rl[n, z].astype(F32)

            @pl.when(z < 3)
            def _():
                with jax.named_scope("last_wait"):
                    remote(sb.at[n, z], rr.at[n, z], snd.at[RS], rz_r.at[n], {"z": z_down}).wait_recv()
                mg[n] = mg[n] + rr[n, z].astype(F32)

            with jax.named_scope("merge"):
                m = mg[n] * (1.0 / TOK) + eb[n]
                mg[n] = m
                lf[outer] = lf[outer] + lax.dot_general(
                    bb[n], m, (((1,), (1,)), ((), ())), precision=lax.Precision.HIGHEST, preferred_element_type=F32
                )

    def lf_copy(i, own):
        o = OUTER_PEERS[i]
        return remote(lf.at[own], lf.at[own], snd.at[LF], got.at[LF], outer_dev(o))

    for i in range(15):
        lf_copy(i, outer).start()

    with jax.named_scope("xx_wait"):
        arrived(xx.at[pl.ds(0, 3)], got.at[XX])
    with jax.named_scope("wc_wait"):
        wc_copy().wait_recv()
    with jax.named_scope("inputs_weight"):
        for h, half in ((core, wy), (1 - core, wo)):
            acc = jnp.zeros((512, SW), F32)
            for j in range(4):
                left = jnp.concatenate([xx[:, ((y + k) % 4) * 4 + j].reshape(512, TOK) for k in range(4)], axis=1)
                acc = acc + jnp.dot(left, half[j].reshape(512, SW), preferred_element_type=F32)
            xo[:, h] = acc.reshape(4, TOK, SW).astype(BF16)
    xw[x] = xo[x]

    with jax.named_scope("lf_wait"):
        arrived(lf.at[pl.ds(0, 15)], got.at[LF])

    with jax.named_scope("gram_schmidt"):
        v = jnp.sum(lf[...], axis=0) * (1.0 / 16)
        rows = lax.broadcasted_iota(jnp.int32, (8, TOK), 0)
        for k in range(8):
            row = v[k:k + 1]
            dots = jnp.sum(v * row, axis=-1, keepdims=True)
            square = dots[k:k + 1] + 1.0
            unit = row / jnp.sqrt(square)
            v = jnp.where(rows > k, v - (dots / square) * row, jnp.where(rows == k, unit, v))
        lall[c] = v

    def la_copy(i, own):
        return remote(lall.at[own], lall.at[own], snd.at[LA], got.at[LA], chip_dev(CHIP_PEERS[i]))

    with jax.named_scope("right_product"):
        vh = v.astype(BF16)
        for n in range(NC):
            rt[n // 2, :, pl.ds((n % 2) * CW, CW)] = jnp.dot(
                vh, mg[n].astype(BF16), preferred_element_type=F32
            ).astype(BF16)

    def rt_copy(i, to, own):
        return remote(rt.at[to % 8], rsb.at[own], snd.at[RT], got.at[RT], outer_dev(OUTER_PEERS[i]))

    for i in range(15):
        rt_copy(i, outer_at(OUTER_PEERS[i]), outer).start()

    rsb[outer] = rt[sl]

    with jax.named_scope("rt_wait"):
        arrived(rsb.at[pl.ds(0, 15)], got.at[RT])

    rall[c, core, 0] = (jnp.sum(rsb[...].astype(F32), axis=0) * (1.0 / 16)).astype(BF16)

    def ro_copy(i):
        _, step, other = OUTER_PEERS[i]
        return remote(
            rall.at[c, core, 0], rall.at[c, core, (4 - step) % 4],
            snd.at[RO], got.at[RO2 if other else RO], outer_dev(OUTER_PEERS[i]),
        )

    for i in range(8, 15):
        ro_copy(i).start()

    def first_copy(i):
        part = rall.at[c, core, 0]
        return remote(part, part, snd.at[RC], got.at[RC], chip_dev(CHIP_PEERS[i]))

    for i in range(15):
        first_copy(i).start()
    for i in (1, 3, 2):
        xo_copy((x + i) % 4).start()
    for i in range(15):
        la_copy(i, c).start()

    def rc_copy(i, own):
        part = rall.at[own, core, pl.ds(1, 3)]
        return remote(part, part, snd.at[RC], rc_r.at[own], chip_dev(CHIP_PEERS[i]))

    def rd_copy(own):
        part = rall.at[own, core]
        return remote(part, part, snd.at[RD], got.at[RD], {"core": 1 - core})

    with jax.named_scope("ro_wait"):
        arrived(rall.at[c, 0, pl.ds(0, 3)], got.at[RO])
    for i in range(15):
        rc_copy(i, c).start()
    with jax.named_scope("ro_wait"):
        arrived(rall.at[c, 0], got.at[RO2])

    with jax.named_scope("new_error"):
        vt = v.T
        vt_hi = vt.astype(BF16)
        vt_lo = (vt - vt_hi.astype(F32)).astype(BF16)
        for i in range(2):
            for r in range(4):
                for half in range(2):
                    n = (((x + r) % 4) * 2 + i) * 2 + half
                    rn = rall[c, i, r, :, pl.ds(half * CW, CW)]
                    approx = jnp.dot(vt_hi, rn, preferred_element_type=F32) + jnp.dot(
                        vt_lo, rn, preferred_element_type=F32
                    )
                    mg[n] = mg[n] - approx
                    columns = pl.ds(pl.multiple_of(n * CW, CW), CW)
                    pltpu.make_async_copy(mg.at[n], ne_hbm.at[0, :, columns], snd.at[NE]).start()

    with jax.named_scope("la_wait"):
        arrived(lall.at[pl.ds(0, 15)], got.at[LA])

    with jax.named_scope("inputs_left"):
        lmat = lall[...].reshape(TOK, TOK)
        lrow = lax.broadcasted_iota(jnp.int32, (TOK, TOK), 0) // 8
        t = jnp.zeros((TOK, TOK), F32)
        for q in range(4):
            lq = jnp.concatenate(
                [jnp.where(lrow == q * 4 + j, lmat, 0.0).astype(BF16) for j in range(4)], axis=1
            )
            xq = jnp.concatenate([xx[x, q * 4 + j] for j in range(4)], axis=1)
            t = t + lax.dot_general(xq, lq, (((1,), (1,)), ((), ())), preferred_element_type=F32)
        t = (t * (-LEARNING_RATE)).astype(BF16)

    with jax.named_scope("rc_wait"):
        arrived(rall.at[pl.ds(0, 15), 0, 0], got.at[RC])
        for i in reversed(range(15)):
            p = chip_at(CHIP_PEERS[i])
            rc_copy(i, p).wait_recv()
            rd_copy(p).start()
    with jax.named_scope("xo_wait"):
        arrived(xo.at[pl.ds(0, 3)], got.at[XO])

    def finish(i):
        for r in range(4):
            n = ((x + r) % 4) * 2 + i
            rn = rall[:, i, r].astype(F32).reshape(TOK, SW).astype(BF16)
            ob[n] = (xw[(x + r) % 4, i].astype(F32) + jnp.dot(t, rn, preferred_element_type=F32)).astype(BF16)
            columns = pl.ds(pl.multiple_of(n * SW, SW), SW)
            pltpu.make_async_copy(ob.at[n], out_hbm.at[:, columns], snd.at[OUT]).start()

    with jax.named_scope("outputs"):
        finish(core)
    with jax.named_scope("rd_wait"):
        arrived(rall.at[pl.ds(0, 15), 0], got.at[RD])
    with jax.named_scope("outputs"):
        finish(1 - core)

    with jax.named_scope("drain"):
        for kind, ref in (
            (WZ, wy.at[pl.ds(0, 3), 0]),
            (WD, wy.at[:, pl.ds(0, 2)]),
            (WR, wy.at[:, 0]),
            (WC, wy),
            (XP, xp.at[pl.ds(0, 2)]),
            (XR, xr),
            (XF, xr.at[pl.ds(0, 3)]),
            (XX, xx.at[pl.ds(0, 3)]),
            (DY, dyb.at[:, pl.ds(0, 2)]),
            (RE, dyb.at[:, 0]),
            (RS, sb.at[:, pl.ds(0, 3)]),
            (LF, lf.at[pl.ds(0, 15)]),
            (LA, lall.at[pl.ds(0, 15)]),
            (RT, rsb.at[pl.ds(0, 15)]),
            (RO, rall.at[pl.ds(0, 7), 0, 0]),
            (RC, rall.at[pl.ds(0, 15), 0]),
            (RD, rall.at[pl.ds(0, 15), 0]),
            (XO, xo.at[pl.ds(0, 3)]),
            (NE, mg),
            (OUT, ob),
        ):
            gone(ref, kind)


def step(inputs, out_grads, weight, start_basis, error_buffer):
    vm = pltpu.VMEM
    dma = pltpu.SemaphoreType.DMA
    return pl.pallas_call(
        body,
        out_shape=(
            jax.ShapeDtypeStruct((TOK, D), BF16),
            jax.ShapeDtypeStruct((1, TOK, D), F32),
        ),
        in_specs=[pl.BlockSpec(memory_space=pl.ANY)] * 5,
        out_specs=(pl.BlockSpec(memory_space=pl.ANY),) * 2,
        scratch_shapes=[
            vm((4, 16, TOK, TOK), BF16),
            vm((4, 4, TOK, TOK), BF16),
            vm((4, TOK, TOK), BF16),
            vm((4, TOK, 512), BF16),
            vm((NC, 4, TOK, CW), BF16),
            vm((4, 4, TOK, SW), BF16),
            vm((4, 4, TOK, SW), BF16),
            vm((NC, TOK, CW), F32),
            vm((NC, 8, CW), F32),
            vm((NC, 4, TOK, CW), F32),
            vm((NC, 4, TOK, CW), BF16),
            vm((NC, 4, TOK, CW), BF16),
            vm((NC, 4, TOK, CW), BF16),
            vm((NC, TOK, CW), F32),
            vm((4, 2, TOK, SW), BF16),
            vm((4, 2, TOK, SW), BF16),
            vm((16, 8, TOK), F32),
            vm((16, 8, TOK), F32),
            vm((NS, 8, SW), BF16),
            vm((16, 8, SW), BF16),
            vm((16, 2, 4, 8, SW), BF16),
            vm((NS, TOK, SW), BF16),
            dma((7,)), dma((20,)), dma((20,)), dma((2, 4)), dma((4,)), dma((4,)), dma((NC,)), dma((NC,)),
            dma((NC, 4)), dma((NC,)), dma((16,)),
        ],
        compiler_params=pltpu.CompilerParams(
            collective_id=0, has_side_effects=True, vmem_limit_bytes=60 * 1024 * 1024
        ),
    )(inputs, out_grads, weight, start_basis, error_buffer)


def solution(mesh):
    finer = Mesh(mesh.devices.reshape(2, 4, 2, 4, 4), AXES)
    outer = ("zh", "x", "core")
    chip = ("y", "z")
    in_specs = (
        P(outer + chip, None),
        P(outer + chip, None),
        P(chip, None),
        P(chip, None),
        P(outer, chip, None),
    )
    out_specs = (P(outer + chip, None), P(outer, chip, None))
    return jax.shard_map(step, mesh=finer, in_specs=in_specs, out_specs=out_specs, check_vma=False)
```

```python
import jax
import jax.numpy as jnp
from jax import lax
from jax.experimental import pallas as pl
from jax.experimental.pallas import tpu as pltpu
from jax.sharding import Mesh
from jax.sharding import PartitionSpec as P

MESH_ID = pl.DeviceIdType.MESH
AXES = ("zh", "x", "core", "y", "z")
LEARNING_RATE = 0.2
TOK = 128
D = 2048
NC = 16
CW = D // NC
NS = 8
SW = D // NS
LAGS = (2, 3)
EARLY = 6
SEMS = 12
WZ, WD, WR, WC, XP, XR, XF, XX, DY, RE, RS, LF, LA, RT, RO, RC, RD, XO, NE, OUT = range(20)
RO2 = 18
OUTER_PEERS = [(h, i, k) for h in (1, 0) for i in (2, 1, 3, 0) for k in (0, 1) if (h, i, k) != (0, 0, 0)]
CHIP_PEERS = [(j, k) for j in (2, 1, 3, 0) for k in (3, 1, 2, 0) if (j, k) != (0, 0)]
F32 = jnp.float32
BF16 = jnp.bfloat16


def body(
    x_hbm, g_hbm, w_hbm, b_hbm, e_hbm, out_hbm, ne_hbm,
    xx, xp, xr, xgt, dyb, wy, wo, eb, bb, pf, sb, rl, rr, mg, xo, xw, lf, lall, rt, rsb, rall, ob,
    ld, snd, got, xp_r, xr_r, wd_r, dy_r, re_r, rs_r, rz_r, rc_r,
):
    zh, x, core, y, z = (lax.axis_index(a) for a in AXES)
    outer = (zh * 4 + x) * 2 + core
    sl = x * 2 + core
    c = y * 4 + z

    def remote(src, dst, ssem, rsem, dev):
        return pltpu.make_async_remote_copy(
            src_ref=src, dst_ref=dst, send_sem=ssem, recv_sem=rsem,
            device_id=dev, device_id_type=MESH_ID,
        )

    def outer_dev(o):
        return {"zh": (zh + o[0]) % 2, "x": (x + o[1]) % 4, "core": (core + o[2]) % 2}

    def outer_at(o):
        dev = outer_dev(o)
        return (dev["zh"] * 4 + dev["x"]) * 2 + dev["core"]

    def chip_dev(k):
        return {"y": (y + k[0]) % 4, "z": (z + k[1]) % 4}

    def chip_at(k):
        dev = chip_dev(k)
        return dev["y"] * 4 + dev["z"]

    ring = ((y + 1) % 4, (y + 3) % 4)
    y2 = (y + 2) % 4
    near = (3, 1)
    goal = (3 - 3 * (z // 2), 2 - z // 2, z + 1 - 2 * (z % 2), z)
    z_up, z_down = (z + 1) % 4, (z + 3) % 4

    def x_load(q, sem):
        return pltpu.make_async_copy(x_hbm.at[:, pl.ds(pl.multiple_of(q * TOK, TOK), TOK)], xx.at[x, q], ld.at[sem])

    def g_load(n, sem):
        return pltpu.make_async_copy(g_hbm.at[:, pl.ds(n * CW, CW)], dyb.at[n, 0], ld.at[sem])

    for k in range(4):
        x_load(k * 4 + goal[0], 0).start()
    for n in range(2):
        g_load(n, 1).start()

    barrier = pltpu.get_barrier_semaphore()
    for dev in OUTER_PEERS:
        pl.semaphore_signal(barrier, inc=1, device_id=outer_dev(dev), device_id_type=MESH_ID)
    for dev in CHIP_PEERS:
        pl.semaphore_signal(barrier, inc=1, device_id=chip_dev(dev), device_id_type=MESH_ID)

    for g in (1, 2, 3):
        for k in range(4):
            x_load(k * 4 + goal[g], 2).start()
    for n in range(2, NC):
        g_load(n, 3).start()
    w_ld = pltpu.make_async_copy(w_hbm.at[:, pl.ds(pl.multiple_of(sl * SW, SW), SW)], wy.at[z, 0], ld.at[4])
    w_ld.start()

    def arrived(ref, sem):
        remote(ref, ref, snd.at[0], sem, {"core": 1 - core}).wait_recv()

    def gone(ref, kind):
        remote(ref, ref, snd.at[kind], got.at[0], {"core": 1 - core}).wait_send()

    arrived(xx.at[x, pl.ds(0, 4)], ld.at[0])
    arrived(dyb.at[pl.ds(0, 2), 0], ld.at[1])
    with jax.named_scope("entry_barrier"):
        pl.semaphore_wait(barrier, 30)

    def wz_copy(p):
        return remote(wy.at[z, 0], wy.at[z, 0], snd.at[WZ], got.at[WZ], {"z": p})

    def wd_copy(way, j):
        return remote(wy.at[j, 0], wy.at[j, near[way]], snd.at[WD], wd_r.at[j], {"y": ring[way]})

    def wr_copy(j, way):
        return remote(wy.at[j, near[way]], wy.at[j, 2], snd.at[WR], got.at[WR], {"y": ring[way]})

    def wc_copy():
        return remote(wy, wo, snd.at[WC], got.at[WC], {"core": 1 - core})

    def xp_copy(way, g):
        p = ring[way]
        return remote(xx.at[x, p * 4 + goal[g]], xp.at[near[way], g], snd.at[XP], xp_r.at[0, g], {"y": p})

    def xr_copy(g):
        return remote(xx.at[x, y2 * 4 + goal[g]], xr.at[g], snd.at[XR], xr_r.at[g], {"y": ring[g % 2]})

    def far_x():
        return remote(xx.at[x, y2 * 4 + goal[0]], xp.at[2, 0], snd.at[XR], xp_r.at[1, 0], {"y": y2})

    def xf_copy(g):
        return remote(xr.at[g], xp.at[2, g], snd.at[XF], xp_r.at[1, g], {"y": ring[g % 2]})

    def xx_copy(p):
        return remote(xx.at[x], xx.at[x], snd.at[XX], got.at[XX], {"x": p})

    def dy_copy(way, n):
        return remote(dyb.at[n, 0], dyb.at[n, near[way]], snd.at[DY], dy_r.at[n % SEMS], {"y": ring[way]})

    def relay(n, way):
        return remote(dyb.at[n, near[way]], dyb.at[n, 2], snd.at[RE], re_r.at[n % SEMS], {"y": ring[way]})

    def direct(n):
        for way in range(2):
            dy_copy(way, n).start()

    def pass_on(n):
        with jax.named_scope("direct_wait"):
            arrived(dyb.at[n, pl.ds(0, 2)], dy_r.at[n % SEMS])
        for way in range(2):
            @pl.when(n % 2 == way)
            def _():
                relay(n, way).start()

    def send_x(g):
        for way in range(2):
            xp_copy(way, g).start()

    def pass_x(g):
        with jax.named_scope("xr_wait"):
            xr_copy(g).wait_recv()
        xf_copy(g).start()

    def gather_x(g, slots):
        with jax.named_scope("xp_wait"):
            if slots == (1, 3):
                arrived(xr.at[pl.ds(0, 2)], xp_r.at[0, g])
            if slots == (2,):
                arrived(xr.at[0], xp_r.at[1, g])
        for k in slots:
            piece = xp[k, g] if k else xx[x, y * 4 + goal[g]]
            xgt[g, :, pl.ds(k * TOK, TOK)] = piece.T

    def product(n, g):
        return jnp.dot(xgt[g], dyb[n].reshape(4 * TOK, CW), preferred_element_type=F32)

    def send_right(n, d):
        cp = remote(sb.at[n, d], rl.at[n, d], snd.at[RS], rs_r.at[n % SEMS, d], {"z": z_up})

        @pl.when(z == 0)
        def _():
            sb[n, d] = pf[n, d].astype(BF16)

        @pl.when(z > 0)
        def _():
            with jax.named_scope("right_wait"):
                cp.wait_recv()
            sb[n, d] = (pf[n, d] + rl[n, d].astype(F32)).astype(BF16)

        cp.start()

    def send_left(n, d, h):
        def copy(sem):
            return remote(sb.at[n, d], rr.at[n, d], snd.at[RS], sem, {"z": z_down})


        @pl.when(z == 3)
        def _():
            sb[n, d] = pf[n, d].astype(BF16)

        @pl.when(z < 3)
        def _():
            with jax.named_scope("left_wait"):
                copy(rs_r.at[n % SEMS, d]).wait_recv()
            sb[n, d] = (pf[n, d] + rr[n, d].astype(F32)).astype(BF16)

        if h > 1:
            copy(rs_r.at[n % SEMS, d]).start()
        else:
            copy(rz_r.at[n % SEMS]).start()

    def xo_copy(p):
        return remote(xo.at[p], xw.at[x], snd.at[XO], got.at[XO], {"x": p})

    far_x().start()
    direct(0)
    send_x(0)
    direct(1)
    arrived(xx.at[x, pl.ds(0, 12)], ld.at[2])
    xr_copy(1).start()
    w_ld.wait()
    for i in range(1, 4):
        wz_copy((z + i) % 4).start()
    for i in (1, 3, 2):
        xx_copy((x + i) % 4).start()
    arrived(dyb.at[pl.ds(0, NC - 2), 0], ld.at[3])
    for n in range(NC):
        pltpu.make_async_copy(b_hbm.at[:, pl.ds(n * CW, CW)], bb.at[n], ld.at[5]).start()
        pltpu.make_async_copy(e_hbm.at[0, :, pl.ds(n * CW, CW)], eb.at[n], ld.at[6]).start()
    gather_x(0, (0,))
    pass_on(0)
    direct(2)
    send_x(1)
    direct(3)
    gather_x(0, (1, 3))
    pass_on(1)
    pass_x(1)
    direct(4)
    gather_x(0, (2,))
    with jax.named_scope("relay_wait"):
        relay(0, 0).wait_recv()
    with jax.named_scope("product"):
        pf[0, goal[0]] = product(0, 0)

    @pl.when(z == 0)
    def _():
        send_right(0, 3)

    @pl.when(z == 3)
    def _():
        send_left(0, 0, 3)

    xr_copy(2).start()
    pass_on(2)
    send_x(2)
    direct(5)
    gather_x(1, (0,))

    arrived(bb, ld.at[5])
    arrived(eb, ld.at[6])
    lf[outer] = jnp.zeros((8, TOK), F32)

    @pl.loop(0, NC + 3 * LAGS[1])
    def _(s):
        @pl.when((s >= 1) & (s + 2 < NC))
        def _():
            pass_on(s + 2)

        @pl.when((s >= 1) & (s + 5 < NC))
        def _():
            direct(s + 5)

        for g in (1, 2, 3):
            @pl.when(s == LAGS[0] * g)
            def _():
                gather_x(g, (1, 3))
                gather_x(g, (2,))

        @pl.when(s == 1)
        def _():
            with jax.named_scope("wz_wait"):
                arrived(wy.at[pl.ds(0, 3), 0], got.at[WZ])

        @pl.when((s >= 11) & (s < 15))
        def _():
            for way in range(2):
                wd_copy(way, s - 11).start()

        for way in range(2):
            @pl.when((s >= 14) & (s < 18) & (s % 2 == way))
            def _():
                j = s - 14
                with jax.named_scope("wd_wait"):
                    arrived(wy.at[j, pl.ds(0, 2)], wd_r.at[j])
                wr_copy(j, way).start()

        @pl.when(s == NC + 4)
        def _():
            with jax.named_scope("wr_wait"):
                arrived(wy.at[:, 2], got.at[WR])
            wc_copy().start()

        @pl.when((s >= 1) & (s < NC))
        def _():
            with jax.named_scope("relay_wait"):
                relay(s, 0).wait_recv()
            with jax.named_scope("product"):
                pf[s, goal[0]] = product(s, 0)

        def turn(k):
            first, later = s - LAGS[0] * k, s - LAGS[1] * k
            n = jnp.where(first < EARLY, first, later)
            return n, (n >= 0) & (n < NC) & ((first < EARLY) | (later >= EARLY))

        for g in (1, 2):
            n, ready = turn(g)

            @pl.when(ready)
            def _():
                with jax.named_scope("product"):
                    pf[n, goal[g]] = product(n, g)

        for h in (3, 2, 1):
            n, ready = turn(3 - h)
            if h == 3:
                ready = ready & (n > 0)

            @pl.when(ready & (z + h < 4))
            def _():
                send_right(n, z + h)

            @pl.when(ready & (z - h >= 0))
            def _():
                send_left(n, z - h, h)

        @pl.when(s == 1)
        def _():
            pass_x(2)
            gather_x(2, (0,))

        @pl.when(s == 2)
        def _():
            xr_copy(3).start()

        @pl.when(s == 3)
        def _():
            send_x(3)
            gather_x(3, (0,))

        @pl.when(s == 4)
        def _():
            pass_x(3)

        last, ready = turn(3)

        @pl.when(ready)
        def _():
            n = last
            mg[n] = product(n, 3)

            @pl.when(z > 0)
            def _():
                with jax.named_scope("last_wait"):
                    remote(sb.at[n, z], rl.at[n, z], snd.at[RS], rs_r.at[n % SEMS, z], {"z": z_up}).wait_recv()
                mg[n] = mg[n] + rl[n, z].astype(F32)

            @pl.when(z < 3)
            def _():
                with jax.named_scope("last_wait"):
                    remote(sb.at[n, z], rr.at[n, z], snd.at[RS], rz_r.at[n % SEMS], {"z": z_down}).wait_recv()
                mg[n] = mg[n] + rr[n, z].astype(F32)

            with jax.named_scope("merge"):
                m = mg[n] * (1.0 / TOK) + eb[n]
                mg[n] = m
                lf[outer] = lf[outer] + lax.dot_general(
                    bb[n], m, (((1,), (1,)), ((), ())), precision=lax.Precision.HIGHEST, preferred_element_type=F32
                )

    def lf_copy(i, own):
        o = OUTER_PEERS[i]
        return remote(lf.at[own], lf.at[own], snd.at[LF], got.at[LF], outer_dev(o))

    for i in range(15):
        lf_copy(i, outer).start()

    with jax.named_scope("xx_wait"):
        arrived(xx.at[pl.ds(0, 3)], got.at[XX])
    with jax.named_scope("wc_wait"):
        wc_copy().wait_recv()
    with jax.named_scope("inputs_weight"):
        for h, half in ((core, wy), (1 - core, wo)):
            acc = jnp.zeros((512, SW), F32)
            for j in range(4):
                left = jnp.concatenate([xx[:, ((y + k) % 4) * 4 + j].reshape(512, TOK) for k in range(4)], axis=1)
                acc = acc + jnp.dot(left, half[j].reshape(512, SW), preferred_element_type=F32)
            xo[:, h] = acc.reshape(4, TOK, SW).astype(BF16)
    xw[x] = xo[x]

    with jax.named_scope("lf_wait"):
        arrived(lf.at[pl.ds(0, 15)], got.at[LF])

    with jax.named_scope("gram_schmidt"):
        v = jnp.sum(lf[...], axis=0) * (1.0 / 16)
        rows = lax.broadcasted_iota(jnp.int32, (8, TOK), 0)
        for k in range(8):
            row = v[k:k + 1]
            dots = jnp.sum(v * row, axis=-1, keepdims=True)
            square = dots[k:k + 1] + 1.0
            unit = row / jnp.sqrt(square)
            v = jnp.where(rows > k, v - (dots / square) * row, jnp.where(rows == k, unit, v))
        lall[c] = v

    def la_copy(i, own):
        return remote(lall.at[own], lall.at[own], snd.at[LA], got.at[LA], chip_dev(CHIP_PEERS[i]))

    with jax.named_scope("right_product"):
        vh = v.astype(BF16)
        for n in range(NC):
            rt[n // 2, :, pl.ds((n % 2) * CW, CW)] = jnp.dot(
                vh, mg[n].astype(BF16), preferred_element_type=F32
            ).astype(BF16)

    def rt_copy(i, to, own):
        return remote(rt.at[to % 8], rsb.at[own], snd.at[RT], got.at[RT], outer_dev(OUTER_PEERS[i]))

    for i in range(15):
        rt_copy(i, outer_at(OUTER_PEERS[i]), outer).start()

    rsb[outer] = rt[sl]

    with jax.named_scope("rt_wait"):
        arrived(rsb.at[pl.ds(0, 15)], got.at[RT])

    rall[c, core, 0] = (jnp.sum(rsb[...].astype(F32), axis=0) * (1.0 / 16)).astype(BF16)

    def ro_copy(i):
        _, step, other = OUTER_PEERS[i]
        return remote(
            rall.at[c, core, 0], rall.at[c, core, (4 - step) % 4],
            snd.at[RO], got.at[RO2 if other else RO], outer_dev(OUTER_PEERS[i]),
        )

    for i in range(8, 15):
        ro_copy(i).start()

    def first_copy(i):
        part = rall.at[c, core, 0]
        return remote(part, part, snd.at[RC], got.at[RC], chip_dev(CHIP_PEERS[i]))

    for i in range(15):
        first_copy(i).start()
    for i in (1, 3, 2):
        xo_copy((x + i) % 4).start()
    for i in range(15):
        la_copy(i, c).start()

    def rc_copy(i, own):
        part = rall.at[own, core, pl.ds(1, 3)]
        return remote(part, part, snd.at[RC], rc_r.at[own], chip_dev(CHIP_PEERS[i]))

    def rd_copy(own):
        part = rall.at[own, core]
        return remote(part, part, snd.at[RD], got.at[RD], {"core": 1 - core})

    with jax.named_scope("ro_wait"):
        arrived(rall.at[c, 0, pl.ds(0, 3)], got.at[RO])
    for i in range(15):
        rc_copy(i, c).start()
    with jax.named_scope("ro_wait"):
        arrived(rall.at[c, 0], got.at[RO2])

    with jax.named_scope("new_error"):
        vt = v.T
        vt_hi = vt.astype(BF16)
        vt_lo = (vt - vt_hi.astype(F32)).astype(BF16)
        for i in range(2):
            for r in range(4):
                for half in range(2):
                    n = (((x + r) % 4) * 2 + i) * 2 + half
                    rn = rall[c, i, r, :, pl.ds(half * CW, CW)]
                    approx = jnp.dot(vt_hi, rn, preferred_element_type=F32) + jnp.dot(
                        vt_lo, rn, preferred_element_type=F32
                    )
                    mg[n] = mg[n] - approx
                    columns = pl.ds(pl.multiple_of(n * CW, CW), CW)
                    pltpu.make_async_copy(mg.at[n], ne_hbm.at[0, :, columns], snd.at[NE]).start()

    with jax.named_scope("la_wait"):
        arrived(lall.at[pl.ds(0, 15)], got.at[LA])

    with jax.named_scope("inputs_left"):
        lmat = lall[...].reshape(TOK, TOK)
        lrow = lax.broadcasted_iota(jnp.int32, (TOK, TOK), 0) // 8
        t = jnp.zeros((TOK, TOK), F32)
        for q in range(4):
            lq = jnp.concatenate(
                [jnp.where(lrow == q * 4 + j, lmat, 0.0).astype(BF16) for j in range(4)], axis=1
            )
            xq = jnp.concatenate([xx[x, q * 4 + j] for j in range(4)], axis=1)
            t = t + lax.dot_general(xq, lq, (((1,), (1,)), ((), ())), preferred_element_type=F32)
        t = (t * (-LEARNING_RATE)).astype(BF16)

    with jax.named_scope("rc_wait"):
        arrived(rall.at[pl.ds(0, 15), 0, 0], got.at[RC])
        for i in reversed(range(15)):
            p = chip_at(CHIP_PEERS[i])
            rc_copy(i, p).wait_recv()
            rd_copy(p).start()
    with jax.named_scope("xo_wait"):
        arrived(xo.at[pl.ds(0, 3)], got.at[XO])

    def finish(i):
        for r in range(4):
            n = ((x + r) % 4) * 2 + i
            rn = rall[:, i, r].astype(F32).reshape(TOK, SW).astype(BF16)
            ob[n] = (xw[(x + r) % 4, i].astype(F32) + jnp.dot(t, rn, preferred_element_type=F32)).astype(BF16)
            columns = pl.ds(pl.multiple_of(n * SW, SW), SW)
            pltpu.make_async_copy(ob.at[n], out_hbm.at[:, columns], snd.at[OUT]).start()

    with jax.named_scope("outputs"):
        finish(core)
    with jax.named_scope("rd_wait"):
        arrived(rall.at[pl.ds(0, 15), 0], got.at[RD])
    with jax.named_scope("outputs"):
        finish(1 - core)

    with jax.named_scope("drain"):
        for kind, ref in (
            (WZ, wy.at[pl.ds(0, 3), 0]),
            (WD, wy.at[:, pl.ds(0, 2)]),
            (WR, wy.at[:, 0]),
            (WC, wy),
            (XP, xp.at[pl.ds(0, 2)]),
            (XR, xr),
            (XF, xr.at[pl.ds(0, 3)]),
            (XX, xx.at[pl.ds(0, 3)]),
            (DY, dyb.at[:, pl.ds(0, 2)]),
            (RE, dyb.at[:, 0]),
            (RS, sb.at[:, pl.ds(0, 3)]),
            (LF, lf.at[pl.ds(0, 15)]),
            (LA, lall.at[pl.ds(0, 15)]),
            (RT, rsb.at[pl.ds(0, 15)]),
            (RO, rall.at[pl.ds(0, 7), 0, 0]),
            (RC, rall.at[pl.ds(0, 15), 0]),
            (RD, rall.at[pl.ds(0, 15), 0]),
            (XO, xo.at[pl.ds(0, 3)]),
            (NE, mg),
            (OUT, ob),
        ):
            gone(ref, kind)


def step(inputs, out_grads, weight, start_basis, error_buffer):
    vm = pltpu.VMEM
    dma = pltpu.SemaphoreType.DMA
    return pl.pallas_call(
        body,
        out_shape=(
            jax.ShapeDtypeStruct((TOK, D), BF16),
            jax.ShapeDtypeStruct((1, TOK, D), F32),
        ),
        in_specs=[pl.BlockSpec(memory_space=pl.ANY)] * 5,
        out_specs=(pl.BlockSpec(memory_space=pl.ANY),) * 2,
        scratch_shapes=[
            vm((4, 16, TOK, TOK), BF16),
            vm((4, 4, TOK, TOK), BF16),
            vm((4, TOK, TOK), BF16),
            vm((4, TOK, 512), BF16),
            vm((NC, 4, TOK, CW), BF16),
            vm((4, 4, TOK, SW), BF16),
            vm((4, 4, TOK, SW), BF16),
            vm((NC, TOK, CW), F32),
            vm((NC, 8, CW), F32),
            vm((NC, 4, TOK, CW), F32),
            vm((NC, 4, TOK, CW), BF16),
            vm((NC, 4, TOK, CW), BF16),
            vm((NC, 4, TOK, CW), BF16),
            vm((NC, TOK, CW), F32),
            vm((4, 2, TOK, SW), BF16),
            vm((4, 2, TOK, SW), BF16),
            vm((16, 8, TOK), F32),
            vm((16, 8, TOK), F32),
            vm((NS, 8, SW), BF16),
            vm((16, 8, SW), BF16),
            vm((16, 2, 4, 8, SW), BF16),
            vm((NS, TOK, SW), BF16),
            dma((7,)), dma((20,)), dma((20,)), dma((2, 4)), dma((4,)), dma((4,)), dma((SEMS,)), dma((SEMS,)),
            dma((SEMS, 4)), dma((SEMS,)), dma((16,)),
        ],
        compiler_params=pltpu.CompilerParams(
            collective_id=0, has_side_effects=True, vmem_limit_bytes=60 * 1024 * 1024
        ),
    )(inputs, out_grads, weight, start_basis, error_buffer)


def solution(mesh):
    finer = Mesh(mesh.devices.reshape(2, 4, 2, 4, 4), AXES)
    outer = ("zh", "x", "core")
    chip = ("y", "z")
    in_specs = (
        P(outer + chip, None),
        P(outer + chip, None),
        P(chip, None),
        P(chip, None),
        P(outer, chip, None),
    )
    out_specs = (P(outer + chip, None), P(outer, chip, None))
    return jax.shard_map(step, mesh=finer, in_specs=in_specs, out_specs=out_specs, check_vma=False)
```
